32 devices in a mesh: gx: 4 (over y, x), gy: 2 (over core), gz: 4 (over z).
Axes of the slice: x: 2, y: 2, z: 4, core: 2. Of those that a mesh axis runs over, the one named last changes fastest.
Arguments:
- energy: float32 [128, 256, 256], P(('gz', 'gy', 'gx')), may hold values from -5 to 5
- flow: float32 [4, 128, 256, 256], P(None, ('gz', 'gy', 'gx')), may hold values from -0.1 to 0.12, as said below
Outputs:
- energy_next: float32 [128, 256, 256], P('gz', 'gx', 'gy')
- plane_mean: float32 [128], P('gz')
- running_mean: float32 [128], P('gz')
The draws below stay inside these ranges and needn't reach their ends.
Inputs may be any that keep to these rules, and one draw needn't show every extreme that they name: flow[0], flow[1] and flow[2] lie within -0.1 to 0.1; flow[3] lies within 0.02 to 0.12.
All inputs are finite; a program needn't handle non-finite values.
Results may differ from the reference program's by a relative error of at most 0.00002.
Values sent between devices are 32-bit elements; how exact they have to be, the bound alone decides.
A program may use at most 128 MiB of HBM per device.

```python
import math
import jax
import jax.numpy as jnp

NX = 256
NY = 256
NZ = 128


def draw_energy(key, part):
    noise_key, phase_key, offset_key = jax.random.split(jax.random.fold_in(key, 11), 3)
    phases = jax.random.uniform(phase_key, (3,), jnp.float32, 0.0, 2.0 * math.pi)
    z_fraction = (jnp.arange(NZ, dtype=jnp.float32) / NZ)[:, None, None]
    x_fraction = (jnp.arange(NX, dtype=jnp.float32) / NX)[None, :, None]
    y_fraction = (jnp.arange(NY, dtype=jnp.float32) / NY)[None, None, :]
    offsets = jax.random.uniform(offset_key, (NZ, 1, 1), jnp.float32, -1.2, 1.2)
    smooth = offsets + 0.6 * jnp.sin(2.0 * math.pi * x_fraction + phases[0]) * jnp.cos(2.0 * math.pi * z_fraction + phases[1]) + 0.3 * jnp.cos(2.0 * math.pi * y_fraction + phases[2])
    noise = 0.8 * jnp.clip(jax.random.normal(noise_key, (NZ, NX, NY), jnp.float32), -3.0, 3.0)
    return (smooth + noise).astype(jnp.float32)


def draw_flow(key, part):
    speed_key, kappa_key = jax.random.split(jax.random.fold_in(key, 23))
    speeds = jax.random.uniform(speed_key, (3, NZ, NX, NY), jnp.float32, -0.1, 0.1)
    conductivity = jnp.exp(jax.random.uniform(kappa_key, (1, NZ, NX, NY), jnp.float32, math.log(0.02), math.log(0.12)))
    return jnp.concatenate([speeds, conductivity], 0).astype(jnp.float32)


def setup_inputs(seed: int = 0) -> dict:
    seeds = jax.random.split(jax.random.key(seed), 3)
    return {
        "energy": draw_energy(jax.random.fold_in(seeds[2], 71), 0),
        "flow": draw_flow(jax.random.fold_in(seeds[2], 71), 0),
    }


directions = ((1, 0, 0), (0, 1, 0), (0, 0, 1))


def extend(field):
    padded = jnp.pad(field, ((0, 0), (1, 1), (1, 1)))
    return jnp.concatenate([padded[-1:], padded, padded[:1]], 0)


def window(array, offset):
    return array[1 + offset[0]: array.shape[0] - 1 + offset[0],
                 1 + offset[1]: array.shape[1] - 1 + offset[1],
                 1 + offset[2]: array.shape[2] - 1 + offset[2]]


def advance(energy_pad, kappa_pad, velocity):
    centre = window(energy_pad, (0, 0, 0))
    kappa_centre = window(kappa_pad, (0, 0, 0))
    change = jnp.zeros_like(centre)
    for axis_number, forward in enumerate(directions):
        backward = tuple(-item for item in forward)
        upper = window(energy_pad, forward)
        lower = window(energy_pad, backward)
        kappa_upper = window(kappa_pad, forward)
        kappa_lower = window(kappa_pad, backward)
        change = change + 0.5 * (kappa_centre + kappa_upper) * (upper - centre) - 0.5 * (kappa_centre + kappa_lower) * (centre - lower)
        speed = velocity[axis_number]
        change = change - jnp.maximum(speed, 0.0) * (centre - lower) - jnp.minimum(speed, 0.0) * (upper - centre)
    return centre + change


def reference(energy, flow):
    velocity = flow[:3]
    kappa_pad = extend(flow[3])
    energy_half = advance(extend(energy), kappa_pad, velocity)
    energy_next = advance(extend(energy_half), kappa_pad, velocity)
    plane_mean = jnp.sum(energy_next, axis=(1, 2)) / (NX * NY)
    ranks = jnp.arange(1, NZ + 1).astype(jnp.float32)
    running_mean = jnp.cumsum(plane_mean) / ranks
    return energy_next, plane_mean, running_mean
```

```python
import functools

import jax
import jax.numpy as jnp
from jax import lax
from jax.experimental import pallas as pl
from jax.experimental.pallas import tpu as pltpu
from jax.sharding import PartitionSpec as P

MESH = pl.DeviceIdType.MESH
PAD = 8
ROWS = 16
STRIP = 32


def shifted(block, rows):
    size = block.shape[0]
    return (
        block[PAD : PAD + rows],
        pltpu.roll(block, size - 1, 0)[PAD : PAD + rows],
        pltpu.roll(block, 1, 0)[PAD : PAD + rows],
    )


def sideways(block, lane):
    width = block.shape[1]
    right = jnp.where(lane == width - 1, 0.0, pltpu.roll(block, width - 1, 1))
    left = jnp.where(lane == 0, 0.0, pltpu.roll(block, 1, 1))
    return right, left


def above(k, k_up, speed, e, e_up):
    return (0.5 * (k + k_up) - jnp.minimum(speed, 0.0)) * (e_up - e)


def below(k, k_down, speed, e, e_down):
    return (0.5 * (k + k_down) + jnp.maximum(speed, 0.0)) * (e_down - e)


def kernel(
    sizes, e_hbm, f_hbm, out, mean_ref, run_ref,
    e_v, k_v, u_v, h_v, n_v, group_v, block_v,
    load_sem, s1, r1, s2, r2, s3, r3, own_sem, s4, r4, s5, r5,
):
    gx_n, gy_n, gz_n, planes, nx, ny = sizes
    height, width = nx // gx_n, ny // gy_n
    gx, gy, gz = lax.axis_index("gx"), lax.axis_index("gy"), lax.axis_index("gz")
    peers = gx_n * gy_n
    place = gy * gx_n + gx
    slab = gz * peers + place

    def device(number):
        return {
            "gx": lax.rem(number, gx_n),
            "gy": lax.rem(lax.div(number, gx_n), gy_n),
            "gz": lax.div(number, peers),
        }

    total = peers * gz_n
    up = device(lax.rem(slab + 1, total))
    down = device(lax.rem(slab + total - 1, total))

    def peer(step):
        return {
            "gx": lax.rem(place + step, gx_n) if gy_n == 1 else lax.rem(lax.rem(place + step, peers), gx_n),
            "gy": lax.div(lax.rem(place + step, peers), gx_n),
            "gz": gz,
        }

    def layer(step):
        return {"gx": gx, "gy": gy, "gz": lax.rem(gz + step, gz_n)}

    loads = [
        pltpu.make_async_copy(e_hbm, e_v.at[pl.ds(1, planes), pl.ds(PAD, nx)], load_sem.at[0]),
        pltpu.make_async_copy(f_hbm.at[3], k_v.at[pl.ds(1, planes), pl.ds(PAD, nx)], load_sem.at[1]),
        pltpu.make_async_copy(f_hbm.at[pl.ds(0, 3)], u_v, load_sem.at[2]),
    ]

    barrier = pltpu.get_barrier_semaphore()
    greet = [up, down] + [peer(i) for i in range(1, peers)] + [layer(i) for i in range(1, gz_n)]
    for target in greet:
        pl.semaphore_signal(barrier, inc=1, device_id=target, device_id_type=MESH)
    for load in loads:
        load.start()
    edge = jnp.zeros((planes, PAD, ny), jnp.float32)
    for ref in (e_v, k_v, h_v):
        ref[1 : planes + 1, 0:PAD, :] = edge
        ref[1 : planes + 1, PAD + nx : PAD + nx + PAD, :] = edge
    pl.semaphore_wait(barrier, len(greet))

    def lanes(c):
        return pl.ds(c * width, width)

    def send(src, dst, send_sem, recv_sem, target):
        return pltpu.make_async_remote_copy(
            src_ref=src, dst_ref=dst, send_sem=send_sem, recv_sem=recv_sem,
            device_id=target, device_id_type=MESH,
        )

    first = []
    rows_all = pl.ds(PAD, nx)
    for c in range(gy_n):
        copies = [
            send(e_hbm.at[planes - 1, :, lanes(c)], e_v.at[0, rows_all, lanes(c)], s1.at[c, 0], r1.at[c, 0], up),
            send(e_hbm.at[0, :, lanes(c)], e_v.at[planes + 1, rows_all, lanes(c)], s1.at[c, 1], r1.at[c, 1], down),
            send(f_hbm.at[3, planes - 1, :, lanes(c)], k_v.at[0, rows_all, lanes(c)], s1.at[c, 2], r1.at[c, 2], up),
            send(f_hbm.at[3, 0, :, lanes(c)], k_v.at[planes + 1, rows_all, lanes(c)], s1.at[c, 3], r1.at[c, 3], down),
        ]
        for copy in copies:
            copy.start()
        first.append(copies)

    for load in loads:
        load.wait()

    lane = lax.broadcasted_iota(jnp.int32, (ROWS, ny), 1)

    def local(src, p, r):
        start = pl.multiple_of(r * ROWS, ROWS)
        here = pl.ds(start, ROWS)
        inner = pl.ds(pl.multiple_of(start + PAD, PAD), ROWS)
        tall = pl.ds(start, ROWS + 2 * PAD)
        e, e_next, e_prev = shifted(src[p + 1, tall, :], ROWS)
        k, k_next, k_prev = shifted(k_v[p + 1, tall, :], ROWS)
        speed = u_v[1, p, here, :]
        value = e + above(k, k_next, speed, e, e_next) + below(k, k_prev, speed, e, e_prev)
        e_next, e_prev = sideways(e, lane)
        k_next, k_prev = sideways(k, lane)
        speed = u_v[2, p, here, :]
        value = value + above(k, k_next, speed, e, e_next) + below(k, k_prev, speed, e, e_prev)
        speed = u_v[0, p, here, :]
        if p < planes - 1:
            value = value + above(k, k_v[p + 2, inner, :], speed, e, src[p + 2, inner, :])
        if p > 0:
            value = value + below(k, k_v[p, inner, :], speed, e, src[p, inner, :])
        return here, inner, value

    def edge_terms(src, c, r):
        start = pl.multiple_of(r * STRIP, STRIP)
        here = pl.ds(start, STRIP)
        inner = pl.ds(pl.multiple_of(start + PAD, PAD), STRIP)
        at = lanes(c)
        top = above(
            k_v[planes, inner, at], k_v[planes + 1, inner, at], u_v[0, planes - 1, here, at],
            src[planes, inner, at], src[planes + 1, inner, at],
        )
        bottom = below(
            k_v[1, inner, at], k_v[0, inner, at], u_v[0, 0, here, at], src[1, inner, at], src[0, inner, at]
        )
        return here, inner, top, bottom

    def folded(value):
        rows = value.shape[0]
        part = value[0:8]
        for i in range(8, rows, 8):
            part = part + value[i : i + 8]
        return part

    for p in range(planes):

        @pl.loop(0, nx // ROWS)
        def _(r, p=p):
            here, inner, value = local(e_v, p, r)
            h_v[p + 1, inner, :] = value

    second = []
    for c in range(gy_n):
        for copy in first[c]:
            copy.wait_recv()

        @pl.loop(0, nx // STRIP)
        def _(r, c=c):
            here, inner, top, bottom = edge_terms(e_v, c, r)
            h_v[planes, inner, lanes(c)] = h_v[planes, inner, lanes(c)] + top
            h_v[1, inner, lanes(c)] = h_v[1, inner, lanes(c)] + bottom

        copies = [
            send(h_v.at[planes, rows_all, lanes(c)], h_v.at[0, rows_all, lanes(c)], s2.at[c, 0], r2.at[c, 0], up),
            send(h_v.at[1, rows_all, lanes(c)], h_v.at[planes + 1, rows_all, lanes(c)], s2.at[c, 1], r2.at[c, 1], down),
        ]
        for copy in copies:
            copy.start()
        second.append(copies)

    sums = []
    for p in range(planes):

        def body(r, carry, p=p):
            here, inner, value = local(h_v, p, r)
            n_v[p, here, :] = value
            return carry + folded(value)

        sums.append(lax.fori_loop(0, nx // ROWS, body, jnp.zeros((8, ny), jnp.float32)))

    def hand_out(c, p0, count, part):
        for d in range(gx_n):
            to = lax.rem(gx + d, gx_n)
            src = n_v.at[pl.ds(p0, count), pl.ds(pl.multiple_of(to * height, 8), height), lanes(c)]
            dst = out.at[pl.ds(place * planes + p0, count)]
            if d == 0:

                @pl.when(gy == c)
                def _():
                    pltpu.make_async_copy(src, dst, own_sem.at[part]).start()

                @pl.when(gy != c)
                def _():
                    send(src, dst, s3.at[c * gx_n + d, part], r3.at[place, part],
                         {"gx": gx, "gy": jnp.int32(c), "gz": gz}).start()
            else:
                send(src, dst, s3.at[c * gx_n + d, part], r3.at[place, part],
                     {"gx": to, "gy": jnp.int32(c), "gz": gz}).start()

    parts = []
    if planes > 2:
        parts.append((1, planes - 2))
        for c in range(gy_n):
            hand_out(c, 1, planes - 2, 0)
    outer = sorted({0, planes - 1})
    first_outer = len(parts)
    parts += [(p, 1) for p in outer]

    extra = [jnp.zeros((8, width), jnp.float32), jnp.zeros((8, width), jnp.float32)]
    for c in range(gy_n):
        for copy in second[c]:
            copy.wait_recv()

        def body(r, carry, c=c):
            here, inner, top, bottom = edge_terms(h_v, c, r)
            n_v[planes - 1, here, lanes(c)] = n_v[planes - 1, here, lanes(c)] + top
            n_v[0, here, lanes(c)] = n_v[0, here, lanes(c)] + bottom
            return carry[0] + folded(top), carry[1] + folded(bottom)

        extra = lax.fori_loop(0, nx // STRIP, body, tuple(extra))
        for part, p in enumerate(outer):
            hand_out(c, p, 1, first_outer + part)

    spot = lax.broadcasted_iota(jnp.int32, (8, 128), 1)
    mine = jnp.zeros((8, 128), jnp.float32)
    for p in range(planes):
        amount = jnp.sum(sums[p], keepdims=True)
        if p == planes - 1:
            amount = amount + jnp.sum(extra[0], keepdims=True)
        if p == 0:
            amount = amount + jnp.sum(extra[1], keepdims=True)
        mine = jnp.where(spot == place * planes + p, amount * (1.0 / (nx * ny)), mine)
    group_v[0] = mine
    share = []
    for i in range(1, peers):
        copy = send(group_v.at[0], group_v.at[i], s4.at[i], r4.at[i], peer(i))
        copy.start()
        share.append(copy)
    for copy in share:
        copy.wait_recv()
    means = mine
    for i in range(1, peers):
        means = means + group_v[i]
    block_v[0] = means
    climb = []
    for i in range(1, gz_n):
        copy = send(block_v.at[0], block_v.at[i], s5.at[i], r5.at[i], layer(i))
        copy.start()
        climb.append(copy)
    running = means
    step = 1
    while step < peers * planes:
        running = running + jnp.where(spot >= step, pltpu.roll(running, step, 1), 0.0)
        step *= 2
    mean_ref[...] = means
    for copy in climb:
        copy.wait_recv()
    lower = jnp.zeros((8, 128), jnp.float32)
    for i in range(1, gz_n):
        lower = lower + jnp.where(gz >= i, block_v[i], 0.0)
    offset = jnp.sum(lower[0:1], axis=1, keepdims=True)
    rank = (gz * peers * planes + spot + 1).astype(jnp.float32)
    run_ref[...] = (running + offset) / rank

    for part, (p0, count) in enumerate(parts):
        for d in range(peers):
            source = lax.rem(place + d, peers)
            dst = out.at[pl.ds(source * planes + p0, count)]
            src = n_v.at[pl.ds(p0, count), pl.ds(0, height), pl.ds(0, width)]
            if d == 0:
                pltpu.make_async_copy(src, dst, own_sem.at[part]).wait()
            else:
                send(src, dst, s3.at[0, part], r3.at[source, part], peer(d)).wait_recv()
        for c in range(gy_n):
            for d in range(gx_n):
                copy = send(
                    n_v.at[pl.ds(p0, count), pl.ds(0, height), pl.ds(0, width)],
                    out.at[pl.ds(p0, count)], s3.at[c * gx_n + d, part], r3.at[0, part], up,
                )
                if d == 0:

                    @pl.when(gy != c)
                    def _():
                        copy.wait_send()
                else:
                    copy.wait_send()
    for copies in first + second + [share, climb]:
        for copy in copies:
            copy.wait_send()


def face_kernel(
    sizes, e_hbm, f_hbm, out, corr, mean_ref, run_ref,
    e_v, k_v, u_v, h_v, n_v, g_v, rx_v, d_v, c_v, near_v, far_v, group_v, block_v,
    load_sem, s1, r1, s2, r2, s3, r3, sc, rc, s4, r4, s5, r5, higher, lower_sem,
):
    gx_n, gy_n, gz_n, planes, nx, ny = sizes
    height, width = nx // gx_n, ny // gy_n
    halves = gx_n // 2
    deep = planes // 2
    gx, gy, gz = lax.axis_index("gx"), lax.axis_index("gy"), lax.axis_index("gz")
    peers = gx_n * gy_n
    count = peers * planes
    place = gy * gx_n + gx
    slab = gz * peers + place
    parity = lax.rem(gx, 2)
    total = peers * gz_n
    last = planes - 1

    def device(number):
        return {
            "gx": lax.rem(number, gx_n),
            "gy": lax.rem(lax.div(number, gx_n), gy_n),
            "gz": lax.div(number, peers),
        }

    def peer(step):
        return device(gz * peers + lax.rem(place + step, peers))

    def layer(step):
        return {"gx": gx, "gy": gy, "gz": lax.rem(gz + step, gz_n)}

    side = (1 - parity, parity)
    sign = tuple((1 - 2 * s).astype(jnp.float32) for s in side)
    far_slab = tuple(lax.rem(slab + total + 2 * s - 1, total) for s in side)
    neighbour = tuple(device(s) for s in far_slab)
    group = tuple(s * deep for s in side)

    def plane(w, t):
        return t + side[w] * (last - 2 * t)

    half_row = lax.div(gx, 2)

    def turn(first, i):
        return lax.rem(first + 1 + i, halves)

    theirs = [2 * turn(half_row, i) + 1 - parity for i in range(halves)]
    mine = [
        [2 * turn(lax.div(lax.rem(far_slab[w], gx_n), 2), i) + parity for i in range(halves)] for w in (0, 1)
    ]

    loads = []
    for w in (0, 1):
        some = pl.ds(group[w], deep)
        loads.append([
            pltpu.make_async_copy(e_hbm.at[some], e_v.at[some, pl.ds(PAD, nx)], load_sem.at[w, 0]),
            pltpu.make_async_copy(f_hbm.at[3, some], k_v.at[some, pl.ds(PAD, nx)], load_sem.at[w, 1]),
            pltpu.make_async_copy(f_hbm.at[pl.ds(0, 3), some], u_v.at[:, some], load_sem.at[w, 2]),
        ])

    barrier = pltpu.get_barrier_semaphore()
    for i in range(1, peers):
        pl.semaphore_signal(barrier, inc=1, device_id=peer(i), device_id_type=MESH)
    for i in range(1, gz_n):

        @pl.when(gz + i < gz_n)
        def _():
            pl.semaphore_signal(barrier, inc=1, device_id=layer(i), device_id_type=MESH)

    for w in (0, 1):
        for load in loads[w]:
            load.start()
    edge = jnp.zeros((planes, PAD, ny), jnp.float32)
    for ref in (e_v, k_v, h_v):
        ref[:, 0:PAD, :] = edge
        ref[:, PAD + nx : PAD + nx + PAD, :] = edge
    pl.semaphore_wait(barrier, peers - 1 + gz)

    def lanes(c):
        return pl.ds(c * width, width)

    def send(src, dst, send_sem, recv_sem, target):
        return pltpu.make_async_remote_copy(
            src_ref=src, dst_ref=dst, send_sem=send_sem, recv_sem=recv_sem,
            device_id=target, device_id_type=MESH,
        )

    def row(block, extra=0):
        return pl.multiple_of(block * height + extra, 8)

    first = {}

    def start_first(w, i, fields):
        p, rows = plane(w, 0), pl.ds(row(theirs[i]), height)
        inner = pl.ds(row(theirs[i], PAD), height)
        sources = (e_hbm.at[p, rows], f_hbm.at[3, p, rows], g_v.at[w, rows], h_v.at[p, inner])
        for field in fields:
            copy = send(
                sources[field], rx_v.at[w, field, i], s1.at[w, field, i], r1.at[w, field, i], neighbour[w]
            )
            copy.start()
            first[w, field, i] = copy

    for i in range(halves):
        start_first(0, i, (0, 1))
    for i in range(1, gz_n):

        @pl.when(gz - i >= 0)
        def _():
            pl.semaphore_signal(higher, inc=1, device_id=layer(gz_n - i), device_id_type=MESH)

    lane = lax.broadcasted_iota(jnp.int32, (ROWS, ny), 1)
    tiles = height // ROWS

    def inplane(src, p, start):
        here = pl.ds(start, ROWS)
        inner = pl.ds(pl.multiple_of(start + PAD, 8), ROWS)
        tall = pl.ds(start, ROWS + 2 * PAD)
        e, e_next, e_prev = shifted(src[p, tall, :], ROWS)
        k, k_next, k_prev = shifted(k_v[p, tall, :], ROWS)
        speed = u_v[1, p, here, :]
        value = e + above(k, k_next, speed, e, e_next) + below(k, k_prev, speed, e, e_prev)
        e_next, e_prev = sideways(e, lane)
        k_next, k_prev = sideways(k, lane)
        speed = u_v[2, p, here, :]
        value = value + above(k, k_next, speed, e, e_next) + below(k, k_prev, speed, e, e_prev)
        return here, inner, value, e, k, u_v[0, p, here, :]

    def at_face(src, w, start):
        p, q = plane(w, 0), plane(w, 1)
        here, inner, value, e, k, speed = inplane(src, p, start)
        speed = sign[w] * speed
        value = value + below(k, k_v[q, inner, :], -speed, e, src[q, inner, :])
        return here, inner, value, k, speed

    def inside(src, p, start):
        here, inner, value, e, k, speed = inplane(src, p, start)
        value = value + above(k, k_v[p + 1, inner, :], speed, e, src[p + 1, inner, :])
        value = value + below(k, k_v[p - 1, inner, :], speed, e, src[p - 1, inner, :])
        return here, inner, value

    def folded(value):
        part = value[0:8]
        for i in range(8, value.shape[0], 8):
            part = part + value[i : i + 8]
        return part

    def first_face(w, block):
        @pl.loop(0, tiles)
        def _(t):
            start = pl.multiple_of(block * height + t * ROWS, 8)
            here, inner, value, k, speed = at_face(e_v, w, start)
            h_v[plane(w, 0), inner, :] = value
            g_v[w, here, :] = 0.5 * k + jnp.maximum(speed, 0.0)

    def first_faces(w):
        for load in loads[w]:
            load.wait()
        for i in range(halves):
            first_face(w, theirs[i])
            start_first(w, i, (2, 3))

    first_faces(0)

    @pl.when(gz < gz_n - 1)
    def _():
        pl.semaphore_wait(higher, gz_n - 1 - gz)

    for i in range(1, gz_n):

        @pl.when(gz + i < gz_n)
        def _():
            pl.semaphore_signal(lower_sem, inc=1, device_id=layer(i), device_id_type=MESH)

    @pl.when(gz > 0)
    def _():
        pl.semaphore_wait(lower_sem, gz)

    for i in range(halves):
        start_first(1, i, (0, 1))
    first_faces(1)
    for w in (0, 1):
        for i in range(halves):
            first_face(w, mine[w][i])
    for p in range(1, last):

        @pl.loop(0, nx // ROWS)
        def _(t, p=p):
            here, inner, value = inside(e_v, p, pl.multiple_of(t * ROWS, 8))
            h_v[p, inner, :] = value

    zero = jnp.zeros((8, ny), jnp.float32)
    spill = [zero, zero]
    sums = [[zero] * deep for _ in (0, 1)]
    second = []

    def second_step(w, t, block, i, low, high):
        def body(r, carry):
            start = pl.multiple_of(block * height + r * ROWS, 8)
            if t == 0:
                here, inner, value, k, speed = at_face(h_v, w, start)
                if i is not None:
                    value = value + near_v[w, i, pl.ds(pl.multiple_of(r * ROWS, 8), ROWS), :]
            else:
                here, inner, value = inside(h_v, plane(w, t), start)
            n_v[plane(w, t), here, :] = value
            return carry + folded(value)

        sums[w][t] = lax.fori_loop(low, high, body, sums[w][t])

    def ahead(w, i):
        for t in range(deep):
            second_step(w, t, mine[w][i], i, 0 if t else 1, tiles if t else tiles - 1)

    def behind(w):
        for i in range(halves):
            for t in sorted({0, tiles - 1}):
                second_step(w, 0, mine[w][i], i, t, t + 1)

    def begin(at_home, src, dst, send_sem, recv_sem, target):
        @pl.when(at_home)
        def _():
            pltpu.make_async_copy(src, dst, recv_sem).start()

        @pl.when(jnp.logical_not(at_home))
        def _():
            send(src, dst, send_sem, recv_sem, target).start()

    def finish(at_home, src, dst, send_sem, recv_sem, target):
        @pl.when(jnp.logical_not(at_home))
        def _():
            send(src, dst, send_sem, recv_sem, target).wait_send()

    def fix_copies(w, i, act):
        far_place, far_block = lax.rem(far_slab[w], peers), lax.div(far_slab[w], peers)
        slot = lax.div(far_place, 2)
        block = mine[w][i]
        for c in range(gy_n):
            at_home = (block == gx) & (gy == c) & (far_block == gz)
            act(
                at_home, far_v.at[w, i, :, lanes(c)], corr.at[slot, 1 - side[w]], sc.at[w, i, c],
                rc.at[slot, 1 - side[w]], {"gx": block, "gy": jnp.int32(c), "gz": far_block},
            )

    def hand_out(w, block, index, act):
        for c in range(gy_n):
            at_home = (block == gx) & (gy == c)
            act(
                at_home, n_v.at[pl.ds(group[w], deep), pl.ds(row(block), height), lanes(c)],
                out.at[pl.ds(place * planes + group[w], deep)],
                s3.at[w, index, c], r3.at[place], {"gx": block, "gy": jnp.int32(c), "gz": gz},
            )

    def meet(w, i):
        for field in range(4):
            send(
                rx_v.at[w, field, i], rx_v.at[w, field, i], s1.at[w, field, i], r1.at[w, field, i], neighbour[w]
            ).wait_recv()
        p = plane(w, 0)

        def body(t, carry):
            at = pl.ds(pl.multiple_of(t * ROWS, 8), ROWS)
            start = pl.multiple_of(mine[w][i] * height + t * ROWS, 8)
            here, inner = pl.ds(start, ROWS), pl.ds(pl.multiple_of(start + PAD, 8), ROWS)
            to_near = g_v[w, here, :] + 0.5 * rx_v[w, 1, i, at, :]
            to_far = rx_v[w, 2, i, at, :] + 0.5 * k_v[p, inner, :]
            step = rx_v[w, 0, i, at, :] - e_v[p, inner, :]
            push = to_far * step
            d_v[w, i, at, :] = -push
            here_half = h_v[p, inner, :] + to_near * step
            far_half = rx_v[w, 3, i, at, :] - push
            h_v[p, inner, :] = here_half
            step = far_half - here_half
            near_v[w, i, at, :] = to_near * step
            fix = -(to_far * step)
            far_v[w, i, at, :] = fix
            return carry + folded(fix)

        spill[w] = lax.fori_loop(0, tiles, body, spill[w])
        copy = send(d_v.at[w, i], c_v.at[w, i], s2.at[w, i], r2.at[w, i], neighbour[w])
        copy.start()
        second.append(copy)
        fix_copies(w, i, begin)

    def give(w, i):
        first[w, 3, i].wait_send()
        send(d_v.at[w, i], c_v.at[w, i], s2.at[w, i], r2.at[w, i], neighbour[w]).wait_recv()
        p = plane(w, 0)

        @pl.loop(0, tiles)
        def _(t):
            at = pl.ds(pl.multiple_of(t * ROWS, 8), ROWS)
            inner = pl.ds(pl.multiple_of(theirs[i] * height + t * ROWS + PAD, 8), ROWS)
            h_v[p, inner, :] = h_v[p, inner, :] + c_v[w, i, at, :]

        for t in range(deep):
            second_step(w, t, theirs[i], None, 0, tiles)

    def hand_theirs(w, i, act):
        hand_out(w, theirs[i], i, act)

    def hand_mine(w, act):
        for i in range(halves):
            hand_out(w, mine[w][i], halves + i, act)

    for i in range(halves):
        meet(0, i)
        ahead(0, i)
    for i in range(halves):
        meet(1, i)
        if i < halves - 1:
            ahead(1, i)
    for i in range(halves):
        give(0, i)
        hand_theirs(0, i, begin)
    behind(0)
    hand_mine(0, begin)
    ahead(1, halves - 1)
    for i in range(halves):
        give(1, i)
    behind(1)

    spot = lax.broadcasted_iota(jnp.int32, (8, 128), 1)
    scale = 1.0 / (nx * ny)
    part = jnp.zeros((8, 128), jnp.float32)
    base = place * planes
    for w in (0, 1):
        part = jnp.where(spot == base + side[w] * (planes + 1), jnp.sum(spill[w], keepdims=True) * scale, part)
        for t in range(deep):
            part = jnp.where(spot == base + 1 + plane(w, t), jnp.sum(sums[w][t], keepdims=True) * scale, part)
    group_v[0] = part
    share = []
    for i in range(1, peers):
        copy = send(group_v.at[0], group_v.at[i], s4.at[i], r4.at[i], peer(i))
        copy.start()
        share.append(copy)
    for i in range(halves):
        hand_theirs(1, i, begin)
    hand_mine(1, begin)
    for copy in share:
        copy.wait_recv()
    for i in range(1, peers):
        part = part + group_v[i]
    block_v[0] = part
    climb = []
    for i in range(1, gz_n):
        copy = send(block_v.at[0], block_v.at[i], s5.at[i], r5.at[i], layer(i))
        copy.start()
        climb.append(copy)
    for copy in climb:
        copy.wait_recv()
    lower = jnp.zeros((8, 128), jnp.float32)
    own_lane = (spot >= 1) & (spot <= count)
    means = jnp.where(own_lane, part, 0.0)
    for i in range(gz_n):
        vector = block_v[i]
        block = lax.rem(gz + gz_n - i, gz_n)
        owner = jnp.where(own_lane, block, jnp.where(
            spot == 0, lax.rem(block + gz_n - 1, gz_n), lax.rem(block + 1, gz_n)))
        vector = jnp.where(spot <= count + 1, vector, 0.0)
        lower = lower + jnp.where(owner < gz, vector, 0.0)
        low = jnp.sum(jnp.where((spot == 0) & (owner == gz), vector, 0.0)[0:1], axis=1, keepdims=True)
        high = jnp.sum(jnp.where((spot == count + 1) & (owner == gz), vector, 0.0)[0:1], axis=1, keepdims=True)
        means = means + jnp.where(spot == count, low, 0.0) + jnp.where(spot == 1, high, 0.0)
    means = pltpu.roll(means, 127, 1)
    running = means
    step = 1
    while step < count:
        running = running + jnp.where(spot >= step, pltpu.roll(running, step, 1), 0.0)
        step *= 2
    mean_ref[...] = means
    offset = jnp.sum(lower[0:1], axis=1, keepdims=True)
    rank = (gz * count + spot + 1).astype(jnp.float32)
    run_ref[...] = (running + offset) / rank

    for s in range(peers):
        dst = out.at[pl.ds(s * planes, planes)]
        send(dst, dst, s3.at[0, 0, 0], r3.at[s], neighbour[0]).wait_recv()
    for slot in range(peers // 2):
        for f in (0, 1):
            send(corr.at[slot, f], corr.at[slot, f], sc.at[0, 0, 0], rc.at[slot, f], neighbour[0]).wait_recv()
    for w in (0, 1):
        for i in range(halves):
            hand_theirs(w, i, finish)
            fix_copies(w, i, finish)
        hand_mine(w, finish)
    for key, copy in first.items():
        if key[1] != 3:
            copy.wait_send()
    for copy in second + share + climb:
        copy.wait_send()


def finish_kernel(planes, base_ref, corr_ref, mean_in, run_in, out_ref, mean_ref, run_ref, fix_v, done):
    other = 1 - lax.rem(lax.axis_index("gx"), 2)
    copies = []
    for slot in range(corr_ref.shape[0]):
        whole = pl.ds((2 * slot + 1 - other) * planes, planes)
        copies.append(pltpu.make_async_copy(base_ref.at[whole], out_ref.at[whole], done.at[slot, 0]))
        copies[-1].start()
    for slot in range(corr_ref.shape[0]):
        start = (2 * slot + other) * planes
        fix_v[slot] = base_ref[pl.ds(start, planes)]
        for f, p in ((0, 0), (1, planes - 1)):
            fix_v[slot, p] = fix_v[slot, p] + corr_ref[slot, f]
        copies.append(pltpu.make_async_copy(fix_v.at[slot], out_ref.at[pl.ds(start, planes)], done.at[slot, 1]))
        copies[-1].start()
    count = mean_ref.shape[0]
    mean_ref[...] = mean_in[0, 0:count]
    run_ref[...] = run_in[0, 0:count]
    for copy in copies:
        copy.wait()


def by_parity(energy, flow):
    gx_n, gy_n, gz_n = (lax.axis_size(a) for a in ("gx", "gy", "gz"))
    planes, nx, ny = energy.shape
    peers, halves = gx_n * gy_n, gx_n // 2
    height, width = nx // gx_n, ny // gy_n
    dma = pltpu.SemaphoreType.DMA
    f32 = jnp.float32
    anywhere = pl.BlockSpec(memory_space=pl.ANY)
    vmem = pl.BlockSpec(memory_space=pltpu.VMEM)
    tall = pltpu.VMEM((planes, nx + 2 * PAD, ny), f32)
    hbm = pl.BlockSpec(memory_space=pltpu.HBM)
    faces = pltpu.VMEM((2, halves, height, ny), f32)
    energy, flow = (pltpu.with_memory_space_constraint(x, pltpu.HBM) for x in (energy, flow))
    base, corr, means, running = pl.pallas_call(
        functools.partial(face_kernel, (gx_n, gy_n, gz_n, planes, nx, ny)),
        out_shape=(
            jax.ShapeDtypeStruct((planes * peers, height, width), f32),
            jax.ShapeDtypeStruct((peers // 2, 2, height, width), f32),
            jax.ShapeDtypeStruct((8, 128), f32),
            jax.ShapeDtypeStruct((8, 128), f32),
        ),
        in_specs=[hbm, hbm],
        out_specs=(anywhere, anywhere, vmem, vmem),
        scratch_shapes=[
            tall, tall, pltpu.VMEM((3, planes, nx, ny), f32), tall,
            pltpu.VMEM((planes, nx, ny), f32), pltpu.VMEM((2, nx, ny), f32),
            pltpu.VMEM((2, 4, halves, height, ny), f32), faces, faces, faces, faces,
            pltpu.VMEM((peers, 8, 128), f32), pltpu.VMEM((gz_n, 8, 128), f32),
            dma((2, 3)), dma((2, 4, halves)), dma((2, 4, halves)), dma((2, halves)), dma((2, halves)),
            dma((2, gx_n, gy_n)), dma((peers,)), dma((2, halves, gy_n)), dma((peers // 2, 2)),
            dma((peers,)), dma((peers,)), dma((gz_n,)), dma((gz_n,)),
            pltpu.SemaphoreType.REGULAR, pltpu.SemaphoreType.REGULAR,
        ],
        compiler_params=pltpu.CompilerParams(
            collective_id=0, has_side_effects=True, vmem_limit_bytes=12 * (energy.size + flow.size)
        ),
    )(energy, flow)
    count = planes * peers
    return tuple(pl.pallas_call(
        functools.partial(finish_kernel, planes),
        out_shape=(
            jax.ShapeDtypeStruct((count, height, width), f32),
            jax.ShapeDtypeStruct((count,), f32),
            jax.ShapeDtypeStruct((count,), f32),
        ),
        in_specs=[vmem] * 4,
        out_specs=(pl.BlockSpec(memory_space=pltpu.HBM), vmem, vmem),
        scratch_shapes=[pltpu.VMEM((peers // 2, planes, height, width), f32), dma((peers // 2, 2))],
        compiler_params=pltpu.CompilerParams(vmem_limit_bytes=12 * (energy.size + flow.size)),
    )(base, corr, means, running))


def per_device(energy, flow):
    gx_n, gy_n, gz_n = (lax.axis_size(a) for a in ("gx", "gy", "gz"))
    planes, nx, ny = energy.shape
    if planes > 3 and planes % 2 == 0 and gx_n % 2 == 0 and gz_n > 1:
        return by_parity(energy, flow)
    peers = gx_n * gy_n
    parts = (1 if planes > 2 else 0) + (2 if planes > 1 else 1)
    dma = pltpu.SemaphoreType.DMA
    f32 = jnp.float32
    anywhere = pl.BlockSpec(memory_space=pl.ANY)
    vmem = pl.BlockSpec(memory_space=pltpu.VMEM)
    tall = pltpu.VMEM((planes + 2, nx + 2 * PAD, ny), f32)
    energy_next, means, running = pl.pallas_call(
        functools.partial(kernel, (gx_n, gy_n, gz_n, planes, nx, ny)),
        out_shape=(
            jax.ShapeDtypeStruct((planes * peers, nx // gx_n, ny // gy_n), f32),
            jax.ShapeDtypeStruct((8, 128), f32),
            jax.ShapeDtypeStruct((8, 128), f32),
        ),
        in_specs=[anywhere, anywhere],
        out_specs=(anywhere, vmem, vmem),
        scratch_shapes=[
            tall, tall, pltpu.VMEM((3, planes, nx, ny), f32), tall,
            pltpu.VMEM((planes, nx, ny), f32),
            pltpu.VMEM((peers, 8, 128), f32), pltpu.VMEM((gz_n, 8, 128), f32),
            dma((3,)), dma((gy_n, 4)), dma((gy_n, 4)), dma((gy_n, 2)), dma((gy_n, 2)),
            dma((peers, parts)), dma((peers, parts)), dma((parts,)),
            dma((peers,)), dma((peers,)), dma((gz_n,)), dma((gz_n,)),
        ],
        compiler_params=pltpu.CompilerParams(collective_id=0, has_side_effects=True),
    )(energy, flow)
    count = planes * peers
    return energy_next, means[0, :count], running[0, :count]


def solution(mesh):
    placed = (P(("gz", "gy", "gx"), None, None), P(None, ("gz", "gy", "gx"), None, None))
    return jax.shard_map(
        per_device,
        mesh=mesh,
        in_specs=placed,
        out_specs=(P("gz", "gx", "gy"), P("gz"), P("gz")),
        check_vma=False,
    )
```

```python
import functools

import jax
import jax.numpy as jnp
from jax import lax
from jax.experimental import pallas as pl
from jax.experimental.pallas import tpu as pltpu
from jax.sharding import PartitionSpec as P

MESH = pl.DeviceIdType.MESH
PAD = 8
ROWS = 16
STRIP = 32


def shifted(block, rows):
    size = block.shape[0]
    return (
        block[PAD : PAD + rows],
        pltpu.roll(block, size - 1, 0)[PAD : PAD + rows],
        pltpu.roll(block, 1, 0)[PAD : PAD + rows],
    )


def sideways(block, lane):
    width = block.shape[1]
    right = jnp.where(lane == width - 1, 0.0, pltpu.roll(block, width - 1, 1))
    left = jnp.where(lane == 0, 0.0, pltpu.roll(block, 1, 1))
    return right, left


def above(k, k_up, speed, e, e_up):
    return (0.5 * (k + k_up) - jnp.minimum(speed, 0.0)) * (e_up - e)


def below(k, k_down, speed, e, e_down):
    return (0.5 * (k + k_down) + jnp.maximum(speed, 0.0)) * (e_down - e)


def kernel(
    sizes, e_hbm, f_hbm, out, mean_ref, run_ref,
    e_v, k_v, u_v, h_v, n_v, group_v, block_v,
    load_sem, s1, r1, s2, r2, s3, r3, own_sem, s4, r4, s5, r5,
):
    gx_n, gy_n, gz_n, planes, nx, ny = sizes
    height, width = nx // gx_n, ny // gy_n
    gx, gy, gz = lax.axis_index("gx"), lax.axis_index("gy"), lax.axis_index("gz")
    peers = gx_n * gy_n
    place = gy * gx_n + gx
    slab = gz * peers + place

    def device(number):
        return {
            "gx": lax.rem(number, gx_n),
            "gy": lax.rem(lax.div(number, gx_n), gy_n),
            "gz": lax.div(number, peers),
        }

    total = peers * gz_n
    up = device(lax.rem(slab + 1, total))
    down = device(lax.rem(slab + total - 1, total))

    def peer(step):
        return {
            "gx": lax.rem(place + step, gx_n) if gy_n == 1 else lax.rem(lax.rem(place + step, peers), gx_n),
            "gy": lax.div(lax.rem(place + step, peers), gx_n),
            "gz": gz,
        }

    def layer(step):
        return {"gx": gx, "gy": gy, "gz": lax.rem(gz + step, gz_n)}

    loads = [
        pltpu.make_async_copy(e_hbm, e_v.at[pl.ds(1, planes), pl.ds(PAD, nx)], load_sem.at[0]),
        pltpu.make_async_copy(f_hbm.at[3], k_v.at[pl.ds(1, planes), pl.ds(PAD, nx)], load_sem.at[1]),
        pltpu.make_async_copy(f_hbm.at[pl.ds(0, 3)], u_v, load_sem.at[2]),
    ]

    barrier = pltpu.get_barrier_semaphore()
    greet = [up, down] + [peer(i) for i in range(1, peers)] + [layer(i) for i in range(1, gz_n)]
    for target in greet:
        pl.semaphore_signal(barrier, inc=1, device_id=target, device_id_type=MESH)
    for load in loads:
        load.start()
    edge = jnp.zeros((planes, PAD, ny), jnp.float32)
    for ref in (e_v, k_v, h_v):
        ref[1 : planes + 1, 0:PAD, :] = edge
        ref[1 : planes + 1, PAD + nx : PAD + nx + PAD, :] = edge
    pl.semaphore_wait(barrier, len(greet))

    def lanes(c):
        return pl.ds(c * width, width)

    def send(src, dst, send_sem, recv_sem, target):
        return pltpu.make_async_remote_copy(
            src_ref=src, dst_ref=dst, send_sem=send_sem, recv_sem=recv_sem,
            device_id=target, device_id_type=MESH,
        )

    first = []
    rows_all = pl.ds(PAD, nx)
    for c in range(gy_n):
        copies = [
            send(e_hbm.at[planes - 1, :, lanes(c)], e_v.at[0, rows_all, lanes(c)], s1.at[c, 0], r1.at[c, 0], up),
            send(e_hbm.at[0, :, lanes(c)], e_v.at[planes + 1, rows_all, lanes(c)], s1.at[c, 1], r1.at[c, 1], down),
            send(f_hbm.at[3, planes - 1, :, lanes(c)], k_v.at[0, rows_all, lanes(c)], s1.at[c, 2], r1.at[c, 2], up),
            send(f_hbm.at[3, 0, :, lanes(c)], k_v.at[planes + 1, rows_all, lanes(c)], s1.at[c, 3], r1.at[c, 3], down),
        ]
        for copy in copies:
            copy.start()
        first.append(copies)

    for load in loads:
        load.wait()

    lane = lax.broadcasted_iota(jnp.int32, (ROWS, ny), 1)

    def local(src, p, r):
        start = pl.multiple_of(r * ROWS, ROWS)
        here = pl.ds(start, ROWS)
        inner = pl.ds(pl.multiple_of(start + PAD, PAD), ROWS)
        tall = pl.ds(start, ROWS + 2 * PAD)
        e, e_next, e_prev = shifted(src[p + 1, tall, :], ROWS)
        k, k_next, k_prev = shifted(k_v[p + 1, tall, :], ROWS)
        speed = u_v[1, p, here, :]
        value = e + above(k, k_next, speed, e, e_next) + below(k, k_prev, speed, e, e_prev)
        e_next, e_prev = sideways(e, lane)
        k_next, k_prev = sideways(k, lane)
        speed = u_v[2, p, here, :]
        value = value + above(k, k_next, speed, e, e_next) + below(k, k_prev, speed, e, e_prev)
        speed = u_v[0, p, here, :]
        if p < planes - 1:
            value = value + above(k, k_v[p + 2, inner, :], speed, e, src[p + 2, inner, :])
        if p > 0:
            value = value + below(k, k_v[p, inner, :], speed, e, src[p, inner, :])
        return here, inner, value

    def edge_terms(src, c, r):
        start = pl.multiple_of(r * STRIP, STRIP)
        here = pl.ds(start, STRIP)
        inner = pl.ds(pl.multiple_of(start + PAD, PAD), STRIP)
        at = lanes(c)
        top = above(
            k_v[planes, inner, at], k_v[planes + 1, inner, at], u_v[0, planes - 1, here, at],
            src[planes, inner, at], src[planes + 1, inner, at],
        )
        bottom = below(
            k_v[1, inner, at], k_v[0, inner, at], u_v[0, 0, here, at], src[1, inner, at], src[0, inner, at]
        )
        return here, inner, top, bottom

    def folded(value):
        rows = value.shape[0]
        part = value[0:8]
        for i in range(8, rows, 8):
            part = part + value[i : i + 8]
        return part

    for p in range(planes):

        @pl.loop(0, nx // ROWS)
        def _(r, p=p):
            here, inner, value = local(e_v, p, r)
            h_v[p + 1, inner, :] = value

    second = []
    for c in range(gy_n):
        for copy in first[c]:
            copy.wait_recv()

        @pl.loop(0, nx // STRIP)
        def _(r, c=c):
            here, inner, top, bottom = edge_terms(e_v, c, r)
            h_v[planes, inner, lanes(c)] = h_v[planes, inner, lanes(c)] + top
            h_v[1, inner, lanes(c)] = h_v[1, inner, lanes(c)] + bottom

        copies = [
            send(h_v.at[planes, rows_all, lanes(c)], h_v.at[0, rows_all, lanes(c)], s2.at[c, 0], r2.at[c, 0], up),
            send(h_v.at[1, rows_all, lanes(c)], h_v.at[planes + 1, rows_all, lanes(c)], s2.at[c, 1], r2.at[c, 1], down),
        ]
        for copy in copies:
            copy.start()
        second.append(copies)

    sums = []
    for p in range(planes):

        def body(r, carry, p=p):
            here, inner, value = local(h_v, p, r)
            n_v[p, here, :] = value
            return carry + folded(value)

        sums.append(lax.fori_loop(0, nx // ROWS, body, jnp.zeros((8, ny), jnp.float32)))

    def hand_out(c, p0, count, part):
        for d in range(gx_n):
            to = lax.rem(gx + d, gx_n)
            src = n_v.at[pl.ds(p0, count), pl.ds(pl.multiple_of(to * height, 8), height), lanes(c)]
            dst = out.at[pl.ds(place * planes + p0, count)]
            if d == 0:

                @pl.when(gy == c)
                def _():
                    pltpu.make_async_copy(src, dst, own_sem.at[part]).start()

                @pl.when(gy != c)
                def _():
                    send(src, dst, s3.at[c * gx_n + d, part], r3.at[place, part],
                         {"gx": gx, "gy": jnp.int32(c), "gz": gz}).start()
            else:
                send(src, dst, s3.at[c * gx_n + d, part], r3.at[place, part],
                     {"gx": to, "gy": jnp.int32(c), "gz": gz}).start()

    parts = []
    if planes > 2:
        parts.append((1, planes - 2))
        for c in range(gy_n):
            hand_out(c, 1, planes - 2, 0)
    outer = sorted({0, planes - 1})
    first_outer = len(parts)
    parts += [(p, 1) for p in outer]

    extra = [jnp.zeros((8, width), jnp.float32), jnp.zeros((8, width), jnp.float32)]
    for c in range(gy_n):
        for copy in second[c]:
            copy.wait_recv()

        def body(r, carry, c=c):
            here, inner, top, bottom = edge_terms(h_v, c, r)
            n_v[planes - 1, here, lanes(c)] = n_v[planes - 1, here, lanes(c)] + top
            n_v[0, here, lanes(c)] = n_v[0, here, lanes(c)] + bottom
            return carry[0] + folded(top), carry[1] + folded(bottom)

        extra = lax.fori_loop(0, nx // STRIP, body, tuple(extra))
        for part, p in enumerate(outer):
            hand_out(c, p, 1, first_outer + part)

    spot = lax.broadcasted_iota(jnp.int32, (8, 128), 1)
    mine = jnp.zeros((8, 128), jnp.float32)
    for p in range(planes):
        amount = jnp.sum(sums[p], keepdims=True)
        if p == planes - 1:
            amount = amount + jnp.sum(extra[0], keepdims=True)
        if p == 0:
            amount = amount + jnp.sum(extra[1], keepdims=True)
        mine = jnp.where(spot == place * planes + p, amount * (1.0 / (nx * ny)), mine)
    group_v[0] = mine
    share = []
    for i in range(1, peers):
        copy = send(group_v.at[0], group_v.at[i], s4.at[i], r4.at[i], peer(i))
        copy.start()
        share.append(copy)
    for copy in share:
        copy.wait_recv()
    means = mine
    for i in range(1, peers):
        means = means + group_v[i]
    block_v[0] = means
    climb = []
    for i in range(1, gz_n):
        copy = send(block_v.at[0], block_v.at[i], s5.at[i], r5.at[i], layer(i))
        copy.start()
        climb.append(copy)
    running = means
    step = 1
    while step < peers * planes:
        running = running + jnp.where(spot >= step, pltpu.roll(running, step, 1), 0.0)
        step *= 2
    mean_ref[...] = means
    for copy in climb:
        copy.wait_recv()
    lower = jnp.zeros((8, 128), jnp.float32)
    for i in range(1, gz_n):
        lower = lower + jnp.where(gz >= i, block_v[i], 0.0)
    offset = jnp.sum(lower[0:1], axis=1, keepdims=True)
    rank = (gz * peers * planes + spot + 1).astype(jnp.float32)
    run_ref[...] = (running + offset) / rank

    for part, (p0, count) in enumerate(parts):
        for d in range(peers):
            source = lax.rem(place + d, peers)
            dst = out.at[pl.ds(source * planes + p0, count)]
            src = n_v.at[pl.ds(p0, count), pl.ds(0, height), pl.ds(0, width)]
            if d == 0:
                pltpu.make_async_copy(src, dst, own_sem.at[part]).wait()
            else:
                send(src, dst, s3.at[0, part], r3.at[source, part], peer(d)).wait_recv()
        for c in range(gy_n):
            for d in range(gx_n):
                copy = send(
                    n_v.at[pl.ds(p0, count), pl.ds(0, height), pl.ds(0, width)],
                    out.at[pl.ds(p0, count)], s3.at[c * gx_n + d, part], r3.at[0, part], up,
                )
                if d == 0:

                    @pl.when(gy != c)
                    def _():
                        copy.wait_send()
                else:
                    copy.wait_send()
    for copies in first + second + [share, climb]:
        for copy in copies:
            copy.wait_send()


def face_kernel(
    sizes, e_hbm, f_hbm, out, mean_ref, run_ref,
    x_v, h_v, n_v, g_v, rx_v, d_v, c_v, near_v, far_v, corr, spill_v, fixed_v, group_v, block_v,
    load_sem, s1, r1, s2, r2, s3, r3, s4, r4, s5, r5, s6, r6, s7, r7, known, higher, lower,
):
    gx_n, gy_n, gz_n, planes, nx, ny = sizes
    height, width = nx // gx_n, ny // gy_n
    halves = gx_n // 2
    deep = planes // 2
    gx, gy, gz = lax.axis_index("gx"), lax.axis_index("gy"), lax.axis_index("gz")
    peers = gx_n * gy_n
    count = peers * planes
    place = gy * gx_n + gx
    slab = gz * peers + place
    parity = lax.rem(gx, 2)
    total = peers * gz_n
    last = planes - 1

    def device(number):
        return {
            "gx": lax.rem(number, gx_n),
            "gy": lax.rem(lax.div(number, gx_n), gy_n),
            "gz": lax.div(number, peers),
        }

    def peer(step):
        return device(gz * peers + lax.rem(place + step, peers))

    def layer(step):
        return {"gx": gx, "gy": gy, "gz": lax.rem(gz + step, gz_n)}

    side = (1 - parity, parity)
    sign = tuple((1 - 2 * s).astype(jnp.float32) for s in side)
    far_slab = tuple(lax.rem(slab + total + 2 * s - 1, total) for s in side)
    neighbour = tuple(device(s) for s in far_slab)
    group = tuple(s * deep for s in side)

    crossing = lax.div(far_slab[1], peers) != gz
    e_v, k_v = x_v.at[0], x_v.at[1]

    def plane(w, t):
        return t + side[w] * (last - 2 * t)

    half_row = lax.div(gx, 2)

    def turn(first, i):
        return lax.rem(first + 1 + i, halves)

    theirs = [2 * turn(half_row, i) + 1 - parity for i in range(halves)]
    mine = [
        [2 * turn(lax.div(lax.rem(far_slab[w], gx_n), 2), i) + parity for i in range(halves)] for w in (0, 1)
    ]

    loads = []
    for w in (0, 1):
        some = pl.ds(group[w], deep)
        loads.append([
            pltpu.make_async_copy(e_hbm.at[some], x_v.at[0, some, pl.ds(PAD, nx)], load_sem.at[w]),
            pltpu.make_async_copy(f_hbm.at[3, some], x_v.at[1, some, pl.ds(PAD, nx)], load_sem.at[w]),
            pltpu.make_async_copy(f_hbm.at[pl.ds(0, 3), some], x_v.at[pl.ds(2, 3), some, pl.ds(PAD, nx)], load_sem.at[w]),
        ])

    barrier = pltpu.get_barrier_semaphore()
    near = [{"gx": gx + 1 - 2 * parity, "gy": gy, "gz": gz}]
    near += [{"gx": lax.rem(gx + 2 * i, gx_n), "gy": gy, "gz": gz} for i in range(1, halves)]
    near += [{"gx": gx, "gy": lax.rem(gy + i, gy_n), "gz": gz} for i in range(1, gy_n)]
    for target in near:
        pl.semaphore_signal(barrier, inc=1, device_id=target, device_id_type=MESH)
    for i in range(1, gz_n):

        @pl.when(gz + i < gz_n)
        def _():
            pl.semaphore_signal(barrier, inc=1, device_id=layer(i), device_id_type=MESH)

    for w in (0, 1):
        for load in loads[w]:
            load.start()
    edge = jnp.zeros((planes, PAD, ny), jnp.float32)
    for ref in (x_v.at[0], x_v.at[1], h_v):
        ref[:, 0:PAD, :] = edge
        ref[:, PAD + nx : PAD + nx + PAD, :] = edge
    block_v[...] = jnp.zeros(block_v.shape, jnp.float32)

    def entry_barrier():
        pl.semaphore_wait(barrier, len(near) + gz)

    entry_barrier()

    def lanes(c):
        return pl.ds(c * width, width)

    def send(src, dst, send_sem, recv_sem, target):
        return pltpu.make_async_remote_copy(
            src_ref=src, dst_ref=dst, send_sem=send_sem, recv_sem=recv_sem,
            device_id=target, device_id_type=MESH,
        )

    def row(block, extra=0):
        return pl.multiple_of(block * height + extra, 8)

    def start_first(w, i, fields):
        p, rows = plane(w, 0), pl.ds(row(theirs[i]), height)
        inner = pl.ds(row(theirs[i], PAD), height)
        sources = (e_hbm.at[p, rows], f_hbm.at[3, p, rows], g_v.at[w, rows], h_v.at[p, inner])
        for field in fields:
            send(sources[field], rx_v.at[w, i, field], s1.at[w], r1.at[w, i], neighbour[w]).start()

    for i in range(halves):
        start_first(0, i, (0, 1))
    for target in near:
        pl.semaphore_signal(known.at[0], inc=1, device_id=target, device_id_type=MESH)

    lane = lax.broadcasted_iota(jnp.int32, (ROWS, ny), 1)
    tiles = height // ROWS

    def inplane(src, p, start):
        here = pl.ds(start, ROWS)
        inner = pl.ds(pl.multiple_of(start + PAD, 8), ROWS)
        tall = pl.ds(start, ROWS + 2 * PAD)
        e, e_next, e_prev = shifted(src[p, tall, :], ROWS)
        k, k_next, k_prev = shifted(k_v[p, tall, :], ROWS)
        speed = x_v[3, p, inner, :]
        value = e + above(k, k_next, speed, e, e_next) + below(k, k_prev, speed, e, e_prev)
        e_next, e_prev = sideways(e, lane)
        k_next, k_prev = sideways(k, lane)
        speed = x_v[4, p, inner, :]
        value = value + above(k, k_next, speed, e, e_next) + below(k, k_prev, speed, e, e_prev)
        return here, inner, value, e, k, x_v[2, p, inner, :]

    def at_face(src, w, start):
        p, q = plane(w, 0), plane(w, 1)
        here, inner, value, e, k, speed = inplane(src, p, start)
        speed = sign[w] * speed
        value = value + below(k, k_v[q, inner, :], -speed, e, src[q, inner, :])
        return here, inner, value, k, speed

    def inside(src, p, start):
        here, inner, value, e, k, speed = inplane(src, p, start)
        value = value + above(k, k_v[p + 1, inner, :], speed, e, src[p + 1, inner, :])
        value = value + below(k, k_v[p - 1, inner, :], speed, e, src[p - 1, inner, :])
        return here, inner, value

    def folded(value):
        part = value[0:8]
        for i in range(8, value.shape[0], 8):
            part = part + value[i : i + 8]
        return part

    def first_face(w, block):
        @pl.loop(0, tiles)
        def _(t):
            start = pl.multiple_of(block * height + t * ROWS, 8)
            here, inner, value, k, speed = at_face(e_v, w, start)
            h_v[plane(w, 0), inner, :] = value
            g_v[w, here, :] = 0.5 * k + jnp.maximum(speed, 0.0)

    def hear_higher():
        @pl.when(gz < gz_n - 1)
        def _():
            pl.semaphore_wait(higher, gz_n - 1 - gz)

        for i in range(1, gz_n):

            @pl.when(gz + i < gz_n)
            def _():
                pl.semaphore_signal(lower, inc=1, device_id=layer(i), device_id_type=MESH)

    def hear_lower():
        @pl.when(gz > 0)
        def _():
            pl.semaphore_wait(lower, gz)

    def land(w):
        some = x_v.at[:, pl.ds(group[w], deep), pl.ds(PAD, nx)]
        pltpu.make_async_copy(some, some, load_sem.at[w]).wait()

    land(0)
    first_face(0, theirs[0])
    start_first(0, 0, (2, 3))
    pl.semaphore_wait(known.at[0], len(near))
    for target in near:
        pl.semaphore_signal(known.at[1], inc=1, device_id=target, device_id_type=MESH)
    for i in range(1, halves):
        first_face(0, theirs[i])
        start_first(0, i, (2, 3))
    land(1)
    first_face(1, theirs[0])
    pl.semaphore_wait(known.at[1], len(near))
    for i in range(1, gz_n):

        @pl.when(gz - i >= 0)
        def _():
            pl.semaphore_signal(higher, inc=1, device_id=layer(gz_n - i), device_id_type=MESH)


    @pl.when(jnp.logical_not(crossing))
    def _():
        start_first(1, 0, (0, 1, 2, 3))

    for i in range(1, halves):
        first_face(1, theirs[i])
    for w in (0, 1):
        for i in range(halves):
            first_face(w, mine[w][i])
    def inner_planes():
        for p in range(1, last):

            @pl.loop(0, nx // ROWS)
            def _(t, p=p):
                here, inner, value = inside(e_v, p, pl.multiple_of(t * ROWS, 8))
                h_v[p, inner, :] = value

    inner_planes()
    hear_higher()

    zero = jnp.zeros((8, ny), jnp.float32)
    spill = [zero, zero]
    sums = [[zero] * deep for _ in (0, 1)]

    def second_step(w, t, block, i, low, high):
        def body(r, carry):
            start = pl.multiple_of(block * height + r * ROWS, 8)
            if t == 0:
                here, inner, value, k, speed = at_face(h_v, w, start)
                if i is not None:
                    value = value + near_v[w, i, pl.ds(pl.multiple_of(r * ROWS, 8), ROWS), :]
            else:
                here, inner, value = inside(h_v, plane(w, t), start)
            n_v[plane(w, t), here, :] = value
            return carry + folded(value)

        sums[w][t] = lax.fori_loop(low, high, body, sums[w][t])

    def ahead(w, i):
        for t in range(deep):
            second_step(w, t, mine[w][i], i, 0 if t else 1, tiles if t else tiles - 1)

    def behind(w):
        for i in range(halves):
            for t in sorted({0, tiles - 1}):
                second_step(w, 0, mine[w][i], i, t, t + 1)

    def begin(at_home, src, dst, send_sem, recv_sem, target):
        @pl.when(at_home)
        def _():
            pltpu.make_async_copy(src, dst, recv_sem).start()

        @pl.when(jnp.logical_not(at_home))
        def _():
            send(src, dst, send_sem, recv_sem, target).start()

    def fix_copies(w, i):
        far_place, far_block = lax.rem(far_slab[w], peers), lax.div(far_slab[w], peers)
        slot = lax.div(far_place, 2)
        block = mine[w][i]
        for c in range(gy_n):
            at_home = (block == gx) & (gy == c) & (far_block == gz)
            begin(
                at_home, far_v.at[w, i, :, lanes(c)], corr.at[slot, 1 - side[w]], s4, r4,
                {"gx": block, "gy": jnp.int32(c), "gz": far_block},
            )

    def meet_wait(w, i):
        send(rx_v.at[w, i], rx_v.at[w, i], s1.at[w], r1.at[w, i], neighbour[w]).wait_recv()

    def meet_calc(w, i):
        p = plane(w, 0)

        def body(t, carry):
            at = pl.ds(pl.multiple_of(t * ROWS, 8), ROWS)
            start = pl.multiple_of(mine[w][i] * height + t * ROWS, 8)
            here, inner = pl.ds(start, ROWS), pl.ds(pl.multiple_of(start + PAD, 8), ROWS)
            to_near = g_v[w, here, :] + 0.5 * rx_v[w, i, 1, at, :]
            to_far = rx_v[w, i, 2, at, :] + 0.5 * k_v[p, inner, :]
            step = rx_v[w, i, 0, at, :] - e_v[p, inner, :]
            push = to_far * step
            d_v[w, i, at, :] = -push
            here_half = h_v[p, inner, :] + to_near * step
            far_half = rx_v[w, i, 3, at, :] - push
            h_v[p, inner, :] = here_half
            step = far_half - here_half
            near_v[w, i, at, :] = to_near * step
            fix = -(to_far * step)
            far_v[w, i, at, :] = fix
            return carry + folded(fix)

        spill[w] = lax.fori_loop(0, tiles, body, spill[w])

    def meet_send(w, i):
        send(d_v.at[w, i], c_v.at[w, i], s2, r2.at[w, i], neighbour[w]).start()
        fix_copies(w, i)

    def spill_copy(w):
        return send(spill_v.at[w], fixed_v.at[w], s5, r5, neighbour[w])

    def spill_out(w):
        spill_v[w] = jnp.broadcast_to(jnp.sum(spill[w], keepdims=True), (8, 128))
        spill_copy(w).start()

    def give_wait(w, i):
        if i == 0:
            send(rx_v.at[w], rx_v.at[w], s1.at[w], r1.at[w, 0], neighbour[w]).wait_send()
        send(d_v.at[w, i], c_v.at[w, i], s2, r2.at[w, i], neighbour[w]).wait_recv()

    def give_calc(w, i):
        p = plane(w, 0)

        @pl.loop(0, tiles)
        def _(t):
            at = pl.ds(pl.multiple_of(t * ROWS, 8), ROWS)
            inner = pl.ds(pl.multiple_of(theirs[i] * height + t * ROWS + PAD, 8), ROWS)
            h_v[p, inner, :] = h_v[p, inner, :] + c_v[w, i, at, :]

        for t in range(deep):
            second_step(w, t, theirs[i], None, 0, tiles)

    def hand_theirs(w, i):
        for c in range(gy_n):
            send(
                n_v.at[pl.ds(group[w], deep), pl.ds(row(theirs[i]), height), lanes(c)],
                out.at[pl.ds(place * planes + group[w], deep)], s3, r3,
                {"gx": theirs[i], "gy": jnp.int32(c), "gz": gz},
            ).start()

    def mine_piece(w, i, p, some, start, rows):
        for c in range(gy_n):
            at_home = (mine[w][i] == gx) & (gy == c)
            begin(
                at_home,
                n_v.at[pl.ds(p, some), pl.ds(row(mine[w][i], start), rows), lanes(c)],
                out.at[pl.ds(place * planes + p, some), pl.ds(start, rows)],
                s3, r3, {"gx": mine[w][i], "gy": jnp.int32(c), "gz": gz},
            )

    def mine_early(w, i):
        mine_piece(w, i, group[w] + 1 - side[w], deep - 1, 0, height)
        mine_piece(w, i, plane(w, 0), 1, ROWS, height - 2 * ROWS)

    def mine_late(w):
        for i in range(halves):
            mine_piece(w, i, plane(w, 0), 1, 0, ROWS)
            mine_piece(w, i, plane(w, 0), 1, height - ROWS, ROWS)

    for i in range(halves):
        meet_wait(0, i)
        meet_calc(0, i)
        meet_send(0, i)
    hear_lower()

    @pl.when(crossing)
    def _():
        start_first(1, 0, (0, 1, 2, 3))

    for i in range(1, halves):
        start_first(1, i, (0, 1, 2, 3))
    spill_out(0)
    for i in range(halves):
        ahead(0, i)
        mine_early(0, i)
    for i in range(halves):
        meet_wait(1, i)
        meet_calc(1, i)
        meet_send(1, i)
        if i < halves - 1:
            ahead(1, i)
            mine_early(1, i)
    spill_out(1)
    for i in range(halves):
        give_wait(0, i)
        give_calc(0, i)
        hand_theirs(0, i)
    behind(0)
    mine_late(0)
    ahead(1, halves - 1)
    mine_early(1, halves - 1)
    for i in range(halves):
        give_wait(1, i)
        give_calc(1, i)
    behind(1)

    spot = lax.broadcasted_iota(jnp.int32, (8, 128), 1)
    scale = 1.0 / (nx * ny)
    part = jnp.zeros((8, 128), jnp.float32)
    send(spill_v, fixed_v, s5, r5, neighbour[0]).wait_recv()
    for w in (0, 1):
        for t in range(deep):
            amount = jnp.sum(sums[w][t], keepdims=True)
            if t == 0:
                amount = amount + fixed_v[w]
            part = jnp.where(spot == place * planes + plane(w, t), amount * scale, part)
    group_v[0] = part
    for i in range(1, peers):
        send(group_v.at[0], group_v.at[i], s6, r6, peer(i)).start()
    for i in range(halves):
        hand_theirs(1, i)
    mine_late(1)

    others = group_v.at[pl.ds(1, peers - 1)]

    def early_sends():
        send(d_v, c_v, s2, r2.at[0, 0], neighbour[0]).wait_send()
        send(spill_v, fixed_v, s5, r5, neighbour[0]).wait_send()

    def share_wait():
        send(others, others, s6, r6, neighbour[0]).wait_recv()

    early_sends()
    share_wait()
    for i in range(1, peers):
        part = part + group_v[i]
    block_v[0] = part

    def climb_copy(i):
        return send(block_v.at[0], block_v.at[i], s7, r7, layer(i))

    for i in range(1, gz_n):

        @pl.when(gz + i < gz_n)
        def _():
            climb_copy(i).start()

    running = part
    step = 1
    while step < count:
        running = running + jnp.where(spot >= step, pltpu.roll(running, step, 1), 0.0)
        step *= 2
    mean_ref[...] = part

    def climb_all():
        for i in range(1, gz_n):

            @pl.when(gz == i)
            def _():
                some = block_v.at[pl.ds(1, i)]
                send(some, some, s7, r7, layer(1)).wait_recv()

    climb_all()
    under = block_v[1]
    for i in range(2, gz_n):
        under = under + block_v[i]
    offset = jnp.sum(jnp.where(spot < count, under, 0.0)[0:1], axis=1, keepdims=True)
    rank = (gz * count + spot + 1).astype(jnp.float32)
    run_ref[...] = (running + offset) / rank

    def final_out():
        send(out, out, s3, r3, neighbour[0]).wait_recv()

    def final_corr():
        send(corr, corr, s4, r4, neighbour[0]).wait_recv()

    final_corr()
    final_out()
    for slot in range(peers // 2):
        start = (2 * slot + 1 - parity) * planes
        for f, p in ((0, 0), (1, last)):
            out[start + p] = out[start + p] + corr[slot, f]

    def final_sends():
        some = out.at[pl.ds(0, (peers - 1) * planes)]
        send(some, some, s3, r3, neighbour[0]).wait_send()
        send(others, others, s6, r6, neighbour[0]).wait_send()
        for n in (0, 1):

            @pl.when(crossing == bool(n))
            def _():
                some = out.at[pl.ds(0, 2 * (halves * gy_n - 1) + n)]
                send(some, some, s4, r4, neighbour[0]).wait_send()

        for i in range(1, gz_n):

            @pl.when(gz == gz_n - 1 - i)
            def _():
                some = block_v.at[pl.ds(0, i)]
                send(some, some, s7, r7, layer(1)).wait_send()

    final_sends()


def finish_kernel(base_ref, mean_in, run_in, out_ref, mean_ref, run_ref, done):
    rows = base_ref.shape[0] // 4
    copies = []
    for i in range(4):
        some = pl.ds(i * rows, rows)
        copies.append(pltpu.make_async_copy(base_ref.at[some], out_ref.at[some], done.at[i]))
        copies[-1].start()
    count = mean_ref.shape[0]
    mean_ref[...] = mean_in[0, 0:count]
    run_ref[...] = run_in[0, 0:count]
    for copy in copies:
        copy.wait()


def by_faces(energy, flow):
    gx_n, gy_n, gz_n = (lax.axis_size(a) for a in ("gx", "gy", "gz"))
    planes, nx, ny = energy.shape
    peers, halves = gx_n * gy_n, gx_n // 2
    height, width = nx // gx_n, ny // gy_n
    dma, regular = pltpu.SemaphoreType.DMA, pltpu.SemaphoreType.REGULAR
    f32 = jnp.float32
    vmem = pl.BlockSpec(memory_space=pltpu.VMEM)
    hbm = pl.BlockSpec(memory_space=pltpu.HBM)
    faces = pltpu.VMEM((2, halves, height, ny), f32)
    energy, flow = (pltpu.with_memory_space_constraint(x, pltpu.HBM) for x in (energy, flow))
    base, means, running = pl.pallas_call(
        functools.partial(face_kernel, (gx_n, gy_n, gz_n, planes, nx, ny)),
        out_shape=(
            jax.ShapeDtypeStruct((planes * peers, height, width), f32),
            jax.ShapeDtypeStruct((8, 128), f32),
            jax.ShapeDtypeStruct((8, 128), f32),
        ),
        in_specs=[hbm, hbm],
        out_specs=(vmem, vmem, vmem),
        scratch_shapes=[
            pltpu.VMEM((5, planes, nx + 2 * PAD, ny), f32), pltpu.VMEM((planes, nx + 2 * PAD, ny), f32),
            pltpu.VMEM((planes, nx, ny), f32), pltpu.VMEM((2, nx, ny), f32),
            pltpu.VMEM((2, halves, 4, height, ny), f32), faces, faces, faces, faces,
            pltpu.VMEM((peers // 2, 2, height, width), f32),
            pltpu.VMEM((2, 8, 128), f32), pltpu.VMEM((2, 8, 128), f32),
            pltpu.VMEM((peers, 8, 128), f32), pltpu.VMEM((gz_n, 8, 128), f32),
            dma((2,)), dma((2,)), dma((2, halves)), dma, dma((2, halves)),
            dma, dma, dma, dma, dma, dma, dma, dma, dma, dma,
            regular((2,)), regular, regular,
        ],
        compiler_params=pltpu.CompilerParams(
            collective_id=0, has_side_effects=True, vmem_limit_bytes=12 * (energy.size + flow.size)
        ),
    )(energy, flow)
    count = planes * peers
    return tuple(pl.pallas_call(
        finish_kernel,
        out_shape=(
            jax.ShapeDtypeStruct((count, height, width), f32),
            jax.ShapeDtypeStruct((count,), f32),
            jax.ShapeDtypeStruct((count,), f32),
        ),
        in_specs=[vmem] * 3,
        out_specs=(pl.BlockSpec(memory_space=pltpu.HBM), vmem, vmem),
        scratch_shapes=[dma((4,))],
        compiler_params=pltpu.CompilerParams(vmem_limit_bytes=12 * (energy.size + flow.size)),
    )(base, means, running))


def per_device(energy, flow):
    gx_n, gy_n, gz_n = (lax.axis_size(a) for a in ("gx", "gy", "gz"))
    planes, nx, ny = energy.shape
    if planes > 3 and planes % 2 == 0 and gx_n % 2 == 0 and gz_n > 1:
        return by_faces(energy, flow)
    peers = gx_n * gy_n
    parts = (1 if planes > 2 else 0) + (2 if planes > 1 else 1)
    dma = pltpu.SemaphoreType.DMA
    f32 = jnp.float32
    anywhere = pl.BlockSpec(memory_space=pl.ANY)
    vmem = pl.BlockSpec(memory_space=pltpu.VMEM)
    tall = pltpu.VMEM((planes + 2, nx + 2 * PAD, ny), f32)
    energy_next, means, running = pl.pallas_call(
        functools.partial(kernel, (gx_n, gy_n, gz_n, planes, nx, ny)),
        out_shape=(
            jax.ShapeDtypeStruct((planes * peers, nx // gx_n, ny // gy_n), f32),
            jax.ShapeDtypeStruct((8, 128), f32),
            jax.ShapeDtypeStruct((8, 128), f32),
        ),
        in_specs=[anywhere, anywhere],
        out_specs=(anywhere, vmem, vmem),
        scratch_shapes=[
            tall, tall, pltpu.VMEM((3, planes, nx, ny), f32), tall,
            pltpu.VMEM((planes, nx, ny), f32),
            pltpu.VMEM((peers, 8, 128), f32), pltpu.VMEM((gz_n, 8, 128), f32),
            dma((3,)), dma((gy_n, 4)), dma((gy_n, 4)), dma((gy_n, 2)), dma((gy_n, 2)),
            dma((peers, parts)), dma((peers, parts)), dma((parts,)),
            dma((peers,)), dma((peers,)), dma((gz_n,)), dma((gz_n,)),
        ],
        compiler_params=pltpu.CompilerParams(collective_id=0, has_side_effects=True),
    )(energy, flow)
    count = planes * peers
    return energy_next, means[0, :count], running[0, :count]


def solution(mesh):
    placed = (P(("gz", "gy", "gx"), None, None), P(None, ("gz", "gy", "gx"), None, None))
    return jax.shard_map(
        per_device,
        mesh=mesh,
        in_specs=placed,
        out_specs=(P("gz", "gx", "gy"), P("gz"), P("gz")),
        check_vma=False,
    )
```

```python
import functools

import jax
import jax.numpy as jnp
from jax import lax
from jax.experimental import pallas as pl
from jax.experimental.pallas import tpu as pltpu
from jax.sharding import PartitionSpec as P

MESH = pl.DeviceIdType.MESH
PAD = 8
ROWS = 16
STRIP = 32


def shifted(block, rows):
    size = block.shape[0]
    return (
        block[PAD : PAD + rows],
        pltpu.roll(block, size - 1, 0)[PAD : PAD + rows],
        pltpu.roll(block, 1, 0)[PAD : PAD + rows],
    )


def sideways(block, lane):
    width = block.shape[1]
    right = jnp.where(lane == width - 1, 0.0, pltpu.roll(block, width - 1, 1))
    left = jnp.where(lane == 0, 0.0, pltpu.roll(block, 1, 1))
    return right, left


def above(k, k_up, speed, e, e_up):
    return (0.5 * (k + k_up) - jnp.minimum(speed, 0.0)) * (e_up - e)


def below(k, k_down, speed, e, e_down):
    return (0.5 * (k + k_down) + jnp.maximum(speed, 0.0)) * (e_down - e)


def kernel(
    sizes, e_hbm, f_hbm, out, mean_ref, run_ref,
    e_v, k_v, u_v, h_v, n_v, group_v, block_v,
    load_sem, s1, r1, s2, r2, s3, r3, own_sem, s4, r4, s5, r5,
):
    gx_n, gy_n, gz_n, planes, nx, ny = sizes
    height, width = nx // gx_n, ny // gy_n
    gx, gy, gz = lax.axis_index("gx"), lax.axis_index("gy"), lax.axis_index("gz")
    peers = gx_n * gy_n
    place = gy * gx_n + gx
    slab = gz * peers + place

    def device(number):
        return {
            "gx": lax.rem(number, gx_n),
            "gy": lax.rem(lax.div(number, gx_n), gy_n),
            "gz": lax.div(number, peers),
        }

    total = peers * gz_n
    up = device(lax.rem(slab + 1, total))
    down = device(lax.rem(slab + total - 1, total))

    def peer(step):
        return {
            "gx": lax.rem(place + step, gx_n) if gy_n == 1 else lax.rem(lax.rem(place + step, peers), gx_n),
            "gy": lax.div(lax.rem(place + step, peers), gx_n),
            "gz": gz,
        }

    def layer(step):
        return {"gx": gx, "gy": gy, "gz": lax.rem(gz + step, gz_n)}

    loads = [
        pltpu.make_async_copy(e_hbm, e_v.at[pl.ds(1, planes), pl.ds(PAD, nx)], load_sem.at[0]),
        pltpu.make_async_copy(f_hbm.at[3], k_v.at[pl.ds(1, planes), pl.ds(PAD, nx)], load_sem.at[1]),
        pltpu.make_async_copy(f_hbm.at[pl.ds(0, 3)], u_v, load_sem.at[2]),
    ]

    barrier = pltpu.get_barrier_semaphore()
    greet = [up, down] + [peer(i) for i in range(1, peers)] + [layer(i) for i in range(1, gz_n)]
    for target in greet:
        pl.semaphore_signal(barrier, inc=1, device_id=target, device_id_type=MESH)
    for load in loads:
        load.start()
    edge = jnp.zeros((planes, PAD, ny), jnp.float32)
    for ref in (e_v, k_v, h_v):
        ref[1 : planes + 1, 0:PAD, :] = edge
        ref[1 : planes + 1, PAD + nx : PAD + nx + PAD, :] = edge
    pl.semaphore_wait(barrier, len(greet))

    def lanes(c):
        return pl.ds(c * width, width)

    def send(src, dst, send_sem, recv_sem, target):
        return pltpu.make_async_remote_copy(
            src_ref=src, dst_ref=dst, send_sem=send_sem, recv_sem=recv_sem,
            device_id=target, device_id_type=MESH,
        )

    first = []
    rows_all = pl.ds(PAD, nx)
    for c in range(gy_n):
        copies = [
            send(e_hbm.at[planes - 1, :, lanes(c)], e_v.at[0, rows_all, lanes(c)], s1.at[c, 0], r1.at[c, 0], up),
            send(e_hbm.at[0, :, lanes(c)], e_v.at[planes + 1, rows_all, lanes(c)], s1.at[c, 1], r1.at[c, 1], down),
            send(f_hbm.at[3, planes - 1, :, lanes(c)], k_v.at[0, rows_all, lanes(c)], s1.at[c, 2], r1.at[c, 2], up),
            send(f_hbm.at[3, 0, :, lanes(c)], k_v.at[planes + 1, rows_all, lanes(c)], s1.at[c, 3], r1.at[c, 3], down),
        ]
        for copy in copies:
            copy.start()
        first.append(copies)

    for load in loads:
        load.wait()

    lane = lax.broadcasted_iota(jnp.int32, (ROWS, ny), 1)

    def local(src, p, r):
        start = pl.multiple_of(r * ROWS, ROWS)
        here = pl.ds(start, ROWS)
        inner = pl.ds(pl.multiple_of(start + PAD, PAD), ROWS)
        tall = pl.ds(start, ROWS + 2 * PAD)
        e, e_next, e_prev = shifted(src[p + 1, tall, :], ROWS)
        k, k_next, k_prev = shifted(k_v[p + 1, tall, :], ROWS)
        speed = u_v[1, p, here, :]
        value = e + above(k, k_next, speed, e, e_next) + below(k, k_prev, speed, e, e_prev)
        e_next, e_prev = sideways(e, lane)
        k_next, k_prev = sideways(k, lane)
        speed = u_v[2, p, here, :]
        value = value + above(k, k_next, speed, e, e_next) + below(k, k_prev, speed, e, e_prev)
        speed = u_v[0, p, here, :]
        if p < planes - 1:
            value = value + above(k, k_v[p + 2, inner, :], speed, e, src[p + 2, inner, :])
        if p > 0:
            value = value + below(k, k_v[p, inner, :], speed, e, src[p, inner, :])
        return here, inner, value

    def edge_terms(src, c, r):
        start = pl.multiple_of(r * STRIP, STRIP)
        here = pl.ds(start, STRIP)
        inner = pl.ds(pl.multiple_of(start + PAD, PAD), STRIP)
        at = lanes(c)
        top = above(
            k_v[planes, inner, at], k_v[planes + 1, inner, at], u_v[0, planes - 1, here, at],
            src[planes, inner, at], src[planes + 1, inner, at],
        )
        bottom = below(
            k_v[1, inner, at], k_v[0, inner, at], u_v[0, 0, here, at], src[1, inner, at], src[0, inner, at]
        )
        return here, inner, top, bottom

    def folded(value):
        rows = value.shape[0]
        part = value[0:8]
        for i in range(8, rows, 8):
            part = part + value[i : i + 8]
        return part

    for p in range(planes):

        @pl.loop(0, nx // ROWS)
        def _(r, p=p):
            here, inner, value = local(e_v, p, r)
            h_v[p + 1, inner, :] = value

    second = []
    for c in range(gy_n):
        for copy in first[c]:
            copy.wait_recv()

        @pl.loop(0, nx // STRIP)
        def _(r, c=c):
            here, inner, top, bottom = edge_terms(e_v, c, r)
            h_v[planes, inner, lanes(c)] = h_v[planes, inner, lanes(c)] + top
            h_v[1, inner, lanes(c)] = h_v[1, inner, lanes(c)] + bottom

        copies = [
            send(h_v.at[planes, rows_all, lanes(c)], h_v.at[0, rows_all, lanes(c)], s2.at[c, 0], r2.at[c, 0], up),
            send(h_v.at[1, rows_all, lanes(c)], h_v.at[planes + 1, rows_all, lanes(c)], s2.at[c, 1], r2.at[c, 1], down),
        ]
        for copy in copies:
            copy.start()
        second.append(copies)

    sums = []
    for p in range(planes):

        def body(r, carry, p=p):
            here, inner, value = local(h_v, p, r)
            n_v[p, here, :] = value
            return carry + folded(value)

        sums.append(lax.fori_loop(0, nx // ROWS, body, jnp.zeros((8, ny), jnp.float32)))

    def hand_out(c, p0, count, part):
        for d in range(gx_n):
            to = lax.rem(gx + d, gx_n)
            src = n_v.at[pl.ds(p0, count), pl.ds(pl.multiple_of(to * height, 8), height), lanes(c)]
            dst = out.at[pl.ds(place * planes + p0, count)]
            if d == 0:

                @pl.when(gy == c)
                def _():
                    pltpu.make_async_copy(src, dst, own_sem.at[part]).start()

                @pl.when(gy != c)
                def _():
                    send(src, dst, s3.at[c * gx_n + d, part], r3.at[place, part],
                         {"gx": gx, "gy": jnp.int32(c), "gz": gz}).start()
            else:
                send(src, dst, s3.at[c * gx_n + d, part], r3.at[place, part],
                     {"gx": to, "gy": jnp.int32(c), "gz": gz}).start()

    parts = []
    if planes > 2:
        parts.append((1, planes - 2))
        for c in range(gy_n):
            hand_out(c, 1, planes - 2, 0)
    outer = sorted({0, planes - 1})
    first_outer = len(parts)
    parts += [(p, 1) for p in outer]

    extra = [jnp.zeros((8, width), jnp.float32), jnp.zeros((8, width), jnp.float32)]
    for c in range(gy_n):
        for copy in second[c]:
            copy.wait_recv()

        def body(r, carry, c=c):
            here, inner, top, bottom = edge_terms(h_v, c, r)
            n_v[planes - 1, here, lanes(c)] = n_v[planes - 1, here, lanes(c)] + top
            n_v[0, here, lanes(c)] = n_v[0, here, lanes(c)] + bottom
            return carry[0] + folded(top), carry[1] + folded(bottom)

        extra = lax.fori_loop(0, nx // STRIP, body, tuple(extra))
        for part, p in enumerate(outer):
            hand_out(c, p, 1, first_outer + part)

    spot = lax.broadcasted_iota(jnp.int32, (8, 128), 1)
    mine = jnp.zeros((8, 128), jnp.float32)
    for p in range(planes):
        amount = jnp.sum(sums[p], keepdims=True)
        if p == planes - 1:
            amount = amount + jnp.sum(extra[0], keepdims=True)
        if p == 0:
            amount = amount + jnp.sum(extra[1], keepdims=True)
        mine = jnp.where(spot == place * planes + p, amount * (1.0 / (nx * ny)), mine)
    group_v[0] = mine
    share = []
    for i in range(1, peers):
        copy = send(group_v.at[0], group_v.at[i], s4.at[i], r4.at[i], peer(i))
        copy.start()
        share.append(copy)
    for copy in share:
        copy.wait_recv()
    means = mine
    for i in range(1, peers):
        means = means + group_v[i]
    block_v[0] = means
    climb = []
    for i in range(1, gz_n):
        copy = send(block_v.at[0], block_v.at[i], s5.at[i], r5.at[i], layer(i))
        copy.start()
        climb.append(copy)
    running = means
    step = 1
    while step < peers * planes:
        running = running + jnp.where(spot >= step, pltpu.roll(running, step, 1), 0.0)
        step *= 2
    mean_ref[...] = means
    for copy in climb:
        copy.wait_recv()
    lower = jnp.zeros((8, 128), jnp.float32)
    for i in range(1, gz_n):
        lower = lower + jnp.where(gz >= i, block_v[i], 0.0)
    offset = jnp.sum(lower[0:1], axis=1, keepdims=True)
    rank = (gz * peers * planes + spot + 1).astype(jnp.float32)
    run_ref[...] = (running + offset) / rank

    for part, (p0, count) in enumerate(parts):
        for d in range(peers):
            source = lax.rem(place + d, peers)
            dst = out.at[pl.ds(source * planes + p0, count)]
            src = n_v.at[pl.ds(p0, count), pl.ds(0, height), pl.ds(0, width)]
            if d == 0:
                pltpu.make_async_copy(src, dst, own_sem.at[part]).wait()
            else:
                send(src, dst, s3.at[0, part], r3.at[source, part], peer(d)).wait_recv()
        for c in range(gy_n):
            for d in range(gx_n):
                copy = send(
                    n_v.at[pl.ds(p0, count), pl.ds(0, height), pl.ds(0, width)],
                    out.at[pl.ds(p0, count)], s3.at[c * gx_n + d, part], r3.at[0, part], up,
                )
                if d == 0:

                    @pl.when(gy != c)
                    def _():
                        copy.wait_send()
                else:
                    copy.wait_send()
    for copies in first + second + [share, climb]:
        for copy in copies:
            copy.wait_send()


def face_kernel(
    sizes, e_hbm, f_hbm, out, mean_ref, run_ref,
    x_v, h_v, n_v, g_v, rx_v, d_v, c_v, near_v, far_v, corr, spill_v, fixed_v, group_v, block_v,
    load_sem, s1, r1, s2, r2, s3, r3, s4, r4, s5, r5, s6, r6, s7, r7, known, higher, lower,
):
    gx_n, gy_n, gz_n, planes, nx, ny = sizes
    height, width = nx // gx_n, ny // gy_n
    halves = gx_n // 2
    deep = planes // 2
    gx, gy, gz = lax.axis_index("gx"), lax.axis_index("gy"), lax.axis_index("gz")
    peers = gx_n * gy_n
    count = peers * planes
    place = gy * gx_n + gx
    slab = gz * peers + place
    parity = lax.rem(gx, 2)
    total = peers * gz_n
    last = planes - 1

    def device(number):
        return {
            "gx": lax.rem(number, gx_n),
            "gy": lax.rem(lax.div(number, gx_n), gy_n),
            "gz": lax.div(number, peers),
        }

    def peer(step):
        return device(gz * peers + lax.rem(place + step, peers))

    def layer(step):
        return {"gx": gx, "gy": gy, "gz": lax.rem(gz + step, gz_n)}

    side = (1 - parity, parity)
    sign = tuple((1 - 2 * s).astype(jnp.float32) for s in side)
    far_slab = tuple(lax.rem(slab + total + 2 * s - 1, total) for s in side)
    neighbour = tuple(device(s) for s in far_slab)
    group = tuple(s * deep for s in side)

    crossing = lax.div(far_slab[1], peers) != gz
    e_v, k_v = x_v.at[0], x_v.at[1]

    def plane(w, t):
        return t + side[w] * (last - 2 * t)

    half_row = lax.div(gx, 2)

    def turn(first, i):
        return lax.rem(first + 1 + i, halves)

    theirs = [2 * turn(half_row, i) + 1 - parity for i in range(halves)]
    mine = [
        [2 * turn(lax.div(lax.rem(far_slab[w], gx_n), 2), i) + parity for i in range(halves)] for w in (0, 1)
    ]

    loads = []
    for w in (0, 1):
        some = pl.ds(group[w], deep)
        loads.append([
            pltpu.make_async_copy(e_hbm.at[some], x_v.at[0, some, pl.ds(PAD, nx)], load_sem.at[w]),
            pltpu.make_async_copy(f_hbm.at[3, some], x_v.at[1, some, pl.ds(PAD, nx)], load_sem.at[w]),
            pltpu.make_async_copy(f_hbm.at[pl.ds(0, 3), some], x_v.at[pl.ds(2, 3), some, pl.ds(PAD, nx)], load_sem.at[w]),
        ])

    barrier = pltpu.get_barrier_semaphore()
    near = [{"gx": gx + 1 - 2 * parity, "gy": gy, "gz": gz}]
    near += [{"gx": lax.rem(gx + 2 * i, gx_n), "gy": gy, "gz": gz} for i in range(1, halves)]
    near += [{"gx": gx, "gy": lax.rem(gy + i, gy_n), "gz": gz} for i in range(1, gy_n)]
    for target in near:
        pl.semaphore_signal(barrier, inc=1, device_id=target, device_id_type=MESH)
    for i in range(1, gz_n):

        @pl.when(gz + i < gz_n)
        def _():
            pl.semaphore_signal(barrier, inc=1, device_id=layer(i), device_id_type=MESH)

    for w in (0, 1):
        for load in loads[w]:
            load.start()
    edge = jnp.zeros((planes, PAD, ny), jnp.float32)
    for ref in (x_v.at[0], x_v.at[1], h_v):
        ref[:, 0:PAD, :] = edge
        ref[:, PAD + nx : PAD + nx + PAD, :] = edge
    block_v[...] = jnp.zeros(block_v.shape, jnp.float32)

    def entry_barrier():
        pl.semaphore_wait(barrier, len(near) + gz)

    entry_barrier()

    def lanes(c):
        return pl.ds(c * width, width)

    def send(src, dst, send_sem, recv_sem, target):
        return pltpu.make_async_remote_copy(
            src_ref=src, dst_ref=dst, send_sem=send_sem, recv_sem=recv_sem,
            device_id=target, device_id_type=MESH,
        )

    def row(block, extra=0):
        return pl.multiple_of(block * height + extra, 8)

    def start_first(w, i, fields):
        p, rows = plane(w, 0), pl.ds(row(theirs[i]), height)
        inner = pl.ds(row(theirs[i], PAD), height)
        sources = (e_hbm.at[p, rows], f_hbm.at[3, p, rows], g_v.at[w, rows], h_v.at[p, inner])
        for field in fields:
            send(sources[field], rx_v.at[w, i, field], s1.at[w], r1.at[w, i], neighbour[w]).start()

    for i in range(halves):
        start_first(0, i, (0, 1))
    for target in near:
        pl.semaphore_signal(known.at[0], inc=1, device_id=target, device_id_type=MESH)

    lane = lax.broadcasted_iota(jnp.int32, (ROWS, ny), 1)
    tiles = height // ROWS

    def inplane(src, p, start):
        here = pl.ds(start, ROWS)
        inner = pl.ds(pl.multiple_of(start + PAD, 8), ROWS)
        tall = pl.ds(start, ROWS + 2 * PAD)
        e, e_next, e_prev = shifted(src[p, tall, :], ROWS)
        k, k_next, k_prev = shifted(k_v[p, tall, :], ROWS)
        speed = x_v[3, p, inner, :]
        value = e + above(k, k_next, speed, e, e_next) + below(k, k_prev, speed, e, e_prev)
        e_next, e_prev = sideways(e, lane)
        k_next, k_prev = sideways(k, lane)
        speed = x_v[4, p, inner, :]
        value = value + above(k, k_next, speed, e, e_next) + below(k, k_prev, speed, e, e_prev)
        return here, inner, value, e, k, x_v[2, p, inner, :]

    def at_face(src, w, start):
        p, q = plane(w, 0), plane(w, 1)
        here, inner, value, e, k, speed = inplane(src, p, start)
        speed = sign[w] * speed
        value = value + below(k, k_v[q, inner, :], -speed, e, src[q, inner, :])
        return here, inner, value, k, speed

    def inside(src, p, start):
        here, inner, value, e, k, speed = inplane(src, p, start)
        value = value + above(k, k_v[p + 1, inner, :], speed, e, src[p + 1, inner, :])
        value = value + below(k, k_v[p - 1, inner, :], speed, e, src[p - 1, inner, :])
        return here, inner, value

    def folded(value):
        part = value[0:8]
        for i in range(8, value.shape[0], 8):
            part = part + value[i : i + 8]
        return part

    def first_face(w, block):
        @pl.loop(0, tiles)
        def _(t):
            start = pl.multiple_of(block * height + t * ROWS, 8)
            here, inner, value, k, speed = at_face(e_v, w, start)
            h_v[plane(w, 0), inner, :] = value
            g_v[w, here, :] = 0.5 * k + jnp.maximum(speed, 0.0)

    def hear_higher():
        @pl.when(gz < gz_n - 1)
        def _():
            pl.semaphore_wait(higher, gz_n - 1 - gz)

        for i in range(1, gz_n):

            @pl.when(gz + i < gz_n)
            def _():
                pl.semaphore_signal(lower, inc=1, device_id=layer(i), device_id_type=MESH)

    def hear_lower():
        @pl.when(gz > 0)
        def _():
            pl.semaphore_wait(lower, gz)

    def land(w):
        some = x_v.at[:, pl.ds(group[w], deep), pl.ds(PAD, nx)]
        pltpu.make_async_copy(some, some, load_sem.at[w]).wait()

    land(0)
    first_face(0, theirs[0])
    start_first(0, 0, (2, 3))
    pl.semaphore_wait(known.at[0], len(near))
    for target in near:
        pl.semaphore_signal(known.at[1], inc=1, device_id=target, device_id_type=MESH)
    for i in range(1, halves):
        first_face(0, theirs[i])
        start_first(0, i, (2, 3))
    land(1)
    first_face(1, theirs[0])
    pl.semaphore_wait(known.at[1], len(near))
    for i in range(1, gz_n):

        @pl.when(gz - i >= 0)
        def _():
            pl.semaphore_signal(higher, inc=1, device_id=layer(gz_n - i), device_id_type=MESH)


    @pl.when(jnp.logical_not(crossing))
    def _():
        start_first(1, 0, (0, 1, 2, 3))

    for i in range(1, halves):
        first_face(1, theirs[i])
    for w in (0, 1):
        for i in range(halves):
            first_face(w, mine[w][i])
    def inner_planes():
        for p in range(1, last):

            @pl.loop(0, nx // ROWS)
            def _(t, p=p):
                here, inner, value = inside(e_v, p, pl.multiple_of(t * ROWS, 8))
                h_v[p, inner, :] = value

    inner_planes()
    hear_higher()

    zero = jnp.zeros((8, ny), jnp.float32)
    spill = [zero, zero]
    sums = [[zero] * deep for _ in (0, 1)]

    def second_step(w, t, block, i, low, high):
        def body(r, carry):
            start = pl.multiple_of(block * height + r * ROWS, 8)
            if t == 0:
                here, inner, value, k, speed = at_face(h_v, w, start)
                if i is not None:
                    value = value + near_v[w, i, pl.ds(pl.multiple_of(r * ROWS, 8), ROWS), :]
            else:
                here, inner, value = inside(h_v, plane(w, t), start)
            n_v[plane(w, t), here, :] = value
            return carry + folded(value)

        sums[w][t] = lax.fori_loop(low, high, body, sums[w][t])

    def ahead(w, i):
        for t in range(deep):
            second_step(w, t, mine[w][i], i, 0 if t else 1, tiles if t else tiles - 1)

    def behind(w):
        for i in range(halves):
            for t in sorted({0, tiles - 1}):
                second_step(w, 0, mine[w][i], i, t, t + 1)

    def begin(at_home, src, dst, send_sem, recv_sem, target):
        @pl.when(at_home)
        def _():
            pltpu.make_async_copy(src, dst, recv_sem).start()

        @pl.when(jnp.logical_not(at_home))
        def _():
            send(src, dst, send_sem, recv_sem, target).start()

    def fix_copies(w, i):
        far_place, far_block = lax.rem(far_slab[w], peers), lax.div(far_slab[w], peers)
        slot = lax.div(far_place, 2)
        block = mine[w][i]
        for c in range(gy_n):
            at_home = (block == gx) & (gy == c) & (far_block == gz)
            begin(
                at_home, far_v.at[w, i, :, lanes(c)], corr.at[slot, 1 - side[w]], s4, r4,
                {"gx": block, "gy": jnp.int32(c), "gz": far_block},
            )

    def meet_wait(w, i):
        send(rx_v.at[w, i], rx_v.at[w, i], s1.at[w], r1.at[w, i], neighbour[w]).wait_recv()

    def meet_calc(w, i):
        p = plane(w, 0)

        def body(t, carry):
            at = pl.ds(pl.multiple_of(t * ROWS, 8), ROWS)
            start = pl.multiple_of(mine[w][i] * height + t * ROWS, 8)
            here, inner = pl.ds(start, ROWS), pl.ds(pl.multiple_of(start + PAD, 8), ROWS)
            to_near = g_v[w, here, :] + 0.5 * rx_v[w, i, 1, at, :]
            to_far = rx_v[w, i, 2, at, :] + 0.5 * k_v[p, inner, :]
            step = rx_v[w, i, 0, at, :] - e_v[p, inner, :]
            push = to_far * step
            d_v[w, i, at, :] = -push
            here_half = h_v[p, inner, :] + to_near * step
            far_half = rx_v[w, i, 3, at, :] - push
            h_v[p, inner, :] = here_half
            step = far_half - here_half
            near_v[w, i, at, :] = to_near * step
            fix = -(to_far * step)
            far_v[w, i, at, :] = fix
            return carry + folded(fix)

        spill[w] = lax.fori_loop(0, tiles, body, spill[w])

    def meet_send(w, i):
        send(d_v.at[w, i], c_v.at[w, i], s2, r2.at[w, i], neighbour[w]).start()
        fix_copies(w, i)

    def spill_copy(w):
        return send(spill_v.at[w, pl.ds(0, 1)], fixed_v.at[w, pl.ds(0, 1)], s5, r5, neighbour[w])

    def spill_out(w):
        spill_v[w] = jnp.broadcast_to(jnp.sum(spill[w], keepdims=True), (8, 128))
        spill_copy(w).start()

    def give_wait(w, i):
        if i == 0:
            send(rx_v.at[w], rx_v.at[w], s1.at[w], r1.at[w, 0], neighbour[w]).wait_send()
        send(d_v.at[w, i], c_v.at[w, i], s2, r2.at[w, i], neighbour[w]).wait_recv()

    def give_calc(w, i):
        p = plane(w, 0)

        @pl.loop(0, tiles)
        def _(t):
            at = pl.ds(pl.multiple_of(t * ROWS, 8), ROWS)
            inner = pl.ds(pl.multiple_of(theirs[i] * height + t * ROWS + PAD, 8), ROWS)
            h_v[p, inner, :] = h_v[p, inner, :] + c_v[w, i, at, :]

        for t in range(deep):
            second_step(w, t, theirs[i], None, 0, tiles)

    def hand_theirs(w, i):
        for c in range(gy_n):
            send(
                n_v.at[pl.ds(group[w], deep), pl.ds(row(theirs[i]), height), lanes(c)],
                out.at[pl.ds(place * planes + group[w], deep)], s3, r3,
                {"gx": theirs[i], "gy": jnp.int32(c), "gz": gz},
            ).start()

    def mine_piece(w, i, p, some, start, rows):
        for c in range(gy_n):
            at_home = (mine[w][i] == gx) & (gy == c)
            begin(
                at_home,
                n_v.at[pl.ds(p, some), pl.ds(row(mine[w][i], start), rows), lanes(c)],
                out.at[pl.ds(place * planes + p, some), pl.ds(start, rows)],
                s3, r3, {"gx": mine[w][i], "gy": jnp.int32(c), "gz": gz},
            )

    def mine_early(w, i):
        mine_piece(w, i, group[w] + 1 - side[w], deep - 1, 0, height)
        mine_piece(w, i, plane(w, 0), 1, ROWS, height - 2 * ROWS)

    def mine_late(w):
        for i in range(halves):
            mine_piece(w, i, plane(w, 0), 1, 0, ROWS)
            mine_piece(w, i, plane(w, 0), 1, height - ROWS, ROWS)

    def when(condition, act):
        @pl.when(condition)
        def _():
            act()

    inland = jnp.logical_not(crossing)

    def second_faces():
        for i in range(1, halves):
            start_first(1, i, (0, 1, 2, 3))

    def hand_first():
        for i in range(halves - 1):
            hand_theirs(0, i)

    for i in range(halves):
        meet_wait(0, i)
        meet_calc(0, i)
        meet_send(0, i)
    hear_lower()
    when(inland, second_faces)
    when(crossing, lambda: start_first(1, 0, (0, 1, 2, 3)))
    spill_out(0)
    for i in range(halves):
        ahead(0, i)
        mine_early(0, i)
    for i in range(halves):
        if i == halves - 1:
            for j in range(halves):
                give_wait(0, j)
                give_calc(0, j)
            when(inland, hand_first)
            behind(0)
            mine_late(0)
        meet_wait(1, i)
        meet_calc(1, i)
        meet_send(1, i)
        if i == 0:
            when(crossing, second_faces)
        if i < halves - 1:
            ahead(1, i)
            mine_early(1, i)
    spill_out(1)
    when(crossing, hand_first)
    hand_theirs(0, halves - 1)
    ahead(1, halves - 1)
    mine_early(1, halves - 1)
    for i in range(halves):
        give_wait(1, i)
        give_calc(1, i)
    behind(1)

    spot = lax.broadcasted_iota(jnp.int32, (1, 128), 1)
    scale = 1.0 / (nx * ny)
    part = jnp.zeros((1, 128), jnp.float32)
    spilled = spill_v.at[:, pl.ds(0, 1)]
    send(spilled, spilled, s5, r5, neighbour[0]).wait_recv()
    for w in (0, 1):
        for t in range(deep):
            amount = jnp.sum(sums[w][t], keepdims=True)
            if t == 0:
                amount = amount + fixed_v[w, 0:1, 0:1]
            part = jnp.where(spot == place * planes + plane(w, t), amount * scale, part)
    group_v[0, 0:1] = part
    for i in range(1, peers):
        send(group_v.at[0, pl.ds(0, 1)], group_v.at[i, pl.ds(0, 1)], s6, r6, peer(i)).start()
    for i in reversed(range(halves)):
        hand_theirs(1, i)
    mine_late(1)

    others = group_v.at[pl.ds(1, peers - 1), pl.ds(0, 1)]

    def early_sends():
        send(d_v, c_v, s2, r2.at[0, 0], neighbour[0]).wait_send()
        send(spilled, spilled, s5, r5, neighbour[0]).wait_send()

    def share_wait():
        send(others, others, s6, r6, neighbour[0]).wait_recv()

    early_sends()
    share_wait()
    for i in range(1, peers):
        part = part + group_v[i, 0:1]
    block_v[0, 0:1] = part

    def climb_copy(i):
        return send(block_v.at[0, pl.ds(0, 1)], block_v.at[i, pl.ds(0, 1)], s7, r7, layer(i))

    for i in range(1, gz_n):

        @pl.when(gz + i < gz_n)
        def _():
            climb_copy(i).start()

    running = part
    step = 1
    while step < count:
        running = running + jnp.where(spot >= step, pltpu.roll(running, step, 1), 0.0)
        step *= 2
    mean_ref[0:1] = part

    def climb_all():
        for i in range(1, gz_n):

            @pl.when(gz == i)
            def _():
                some = block_v.at[pl.ds(1, i), pl.ds(0, 1)]
                send(some, some, s7, r7, layer(1)).wait_recv()

    climb_all()
    under = block_v[1, 0:1]
    for i in range(2, gz_n):
        under = under + block_v[i, 0:1]
    offset = jnp.sum(jnp.where(spot < count, under, 0.0), axis=1, keepdims=True)
    rank = (gz * count + spot + 1).astype(jnp.float32)
    run_ref[0:1] = (running + offset) / rank

    def final_out():
        send(out, out, s3, r3, neighbour[0]).wait_recv()

    def final_corr():
        send(corr, corr, s4, r4, neighbour[0]).wait_recv()

    final_corr()
    final_out()
    for slot in range(peers // 2):
        start = (2 * slot + 1 - parity) * planes
        for f, p in ((0, 0), (1, last)):
            out[start + p] = out[start + p] + corr[slot, f]

    def final_sends():
        some = out.at[pl.ds(0, (peers - 1) * planes)]
        send(some, some, s3, r3, neighbour[0]).wait_send()
        send(others, others, s6, r6, neighbour[0]).wait_send()
        for n in (0, 1):

            @pl.when(crossing == bool(n))
            def _():
                some = out.at[pl.ds(0, 2 * (halves * gy_n - 1) + n)]
                send(some, some, s4, r4, neighbour[0]).wait_send()

        for i in range(1, gz_n):

            @pl.when(gz == gz_n - 1 - i)
            def _():
                some = block_v.at[pl.ds(0, i), pl.ds(0, 1)]
                send(some, some, s7, r7, layer(1)).wait_send()

    final_sends()


def finish_kernel(base_ref, mean_in, run_in, out_ref, mean_ref, run_ref, mean_v, run_v, done):
    copies = [pltpu.make_async_copy(base_ref, out_ref, done.at[0])]
    copies[0].start()
    count = mean_ref.shape[0]
    for source, staged, target, i in ((mean_in, mean_v, mean_ref, 1), (run_in, run_v, run_ref, 2)):
        staged[...] = source[0, 0:count]
        copies.append(pltpu.make_async_copy(staged, target, done.at[i]))
        copies[i].start()
    for copy in copies:
        copy.wait()


def by_faces(energy, flow):
    gx_n, gy_n, gz_n = (lax.axis_size(a) for a in ("gx", "gy", "gz"))
    planes, nx, ny = energy.shape
    peers, halves = gx_n * gy_n, gx_n // 2
    height, width = nx // gx_n, ny // gy_n
    dma, regular = pltpu.SemaphoreType.DMA, pltpu.SemaphoreType.REGULAR
    f32 = jnp.float32
    vmem = pl.BlockSpec(memory_space=pltpu.VMEM)
    hbm = pl.BlockSpec(memory_space=pltpu.HBM)
    faces = pltpu.VMEM((2, halves, height, ny), f32)
    energy, flow = (pltpu.with_memory_space_constraint(x, pltpu.HBM) for x in (energy, flow))
    base, means, running = pl.pallas_call(
        functools.partial(face_kernel, (gx_n, gy_n, gz_n, planes, nx, ny)),
        out_shape=(
            jax.ShapeDtypeStruct((planes * peers, height, width), f32),
            jax.ShapeDtypeStruct((8, 128), f32),
            jax.ShapeDtypeStruct((8, 128), f32),
        ),
        in_specs=[hbm, hbm],
        out_specs=(vmem, vmem, vmem),
        scratch_shapes=[
            pltpu.VMEM((5, planes, nx + 2 * PAD, ny), f32), pltpu.VMEM((planes, nx + 2 * PAD, ny), f32),
            pltpu.VMEM((planes, nx, ny), f32), pltpu.VMEM((2, nx, ny), f32),
            pltpu.VMEM((2, halves, 4, height, ny), f32), faces, faces, faces, faces,
            pltpu.VMEM((peers // 2, 2, height, width), f32),
            pltpu.VMEM((2, 8, 128), f32), pltpu.VMEM((2, 8, 128), f32),
            pltpu.VMEM((peers, 8, 128), f32), pltpu.VMEM((gz_n, 8, 128), f32),
            dma((2,)), dma((2,)), dma((2, halves)), dma, dma((2, halves)),
            dma, dma, dma, dma, dma, dma, dma, dma, dma, dma,
            regular((2,)), regular, regular,
        ],
        compiler_params=pltpu.CompilerParams(
            collective_id=0, has_side_effects=True, vmem_limit_bytes=12 * (energy.size + flow.size)
        ),
    )(energy, flow)
    count = planes * peers
    return tuple(pl.pallas_call(
        finish_kernel,
        out_shape=(
            jax.ShapeDtypeStruct((count, height, width), f32),
            jax.ShapeDtypeStruct((count,), f32),
            jax.ShapeDtypeStruct((count,), f32),
        ),
        in_specs=[vmem] * 3,
        out_specs=(hbm, hbm, hbm),
        scratch_shapes=[pltpu.VMEM((count,), f32), pltpu.VMEM((count,), f32), dma((3,))],
        compiler_params=pltpu.CompilerParams(vmem_limit_bytes=12 * (energy.size + flow.size)),
    )(base, means, running))


def per_device(energy, flow):
    gx_n, gy_n, gz_n = (lax.axis_size(a) for a in ("gx", "gy", "gz"))
    planes, nx, ny = energy.shape
    if planes > 3 and planes % 2 == 0 and gx_n % 2 == 0 and gz_n > 1:
        return by_faces(energy, flow)
    peers = gx_n * gy_n
    parts = (1 if planes > 2 else 0) + (2 if planes > 1 else 1)
    dma = pltpu.SemaphoreType.DMA
    f32 = jnp.float32
    anywhere = pl.BlockSpec(memory_space=pl.ANY)
    vmem = pl.BlockSpec(memory_space=pltpu.VMEM)
    tall = pltpu.VMEM((planes + 2, nx + 2 * PAD, ny), f32)
    energy_next, means, running = pl.pallas_call(
        functools.partial(kernel, (gx_n, gy_n, gz_n, planes, nx, ny)),
        out_shape=(
            jax.ShapeDtypeStruct((planes * peers, nx // gx_n, ny // gy_n), f32),
            jax.ShapeDtypeStruct((8, 128), f32),
            jax.ShapeDtypeStruct((8, 128), f32),
        ),
        in_specs=[anywhere, anywhere],
        out_specs=(anywhere, vmem, vmem),
        scratch_shapes=[
            tall, tall, pltpu.VMEM((3, planes, nx, ny), f32), tall,
            pltpu.VMEM((planes, nx, ny), f32),
            pltpu.VMEM((peers, 8, 128), f32), pltpu.VMEM((gz_n, 8, 128), f32),
            dma((3,)), dma((gy_n, 4)), dma((gy_n, 4)), dma((gy_n, 2)), dma((gy_n, 2)),
            dma((peers, parts)), dma((peers, parts)), dma((parts,)),
            dma((peers,)), dma((peers,)), dma((gz_n,)), dma((gz_n,)),
        ],
        compiler_params=pltpu.CompilerParams(collective_id=0, has_side_effects=True),
    )(energy, flow)
    count = planes * peers
    return energy_next, means[0, :count], running[0, :count]


def solution(mesh):
    placed = (P(("gz", "gy", "gx"), None, None), P(None, ("gz", "gy", "gx"), None, None))
    return jax.shard_map(
        per_device,
        mesh=mesh,
        in_specs=placed,
        out_specs=(P("gz", "gx", "gy"), P("gz"), P("gz")),
        check_vma=False,
    )
```

```python
import functools

import jax
import jax.numpy as jnp
from jax import lax
from jax.experimental import pallas as pl
from jax.experimental.pallas import tpu as pltpu
from jax.sharding import PartitionSpec as P

MESH = pl.DeviceIdType.MESH
PAD = 8
ROWS = 16
STRIP = 32


def shifted(block, rows):
    size = block.shape[0]
    return (
        block[PAD : PAD + rows],
        pltpu.roll(block, size - 1, 0)[PAD : PAD + rows],
        pltpu.roll(block, 1, 0)[PAD : PAD + rows],
    )


def sideways(block, lane):
    width = block.shape[1]
    right = jnp.where(lane == width - 1, 0.0, pltpu.roll(block, width - 1, 1))
    left = jnp.where(lane == 0, 0.0, pltpu.roll(block, 1, 1))
    return right, left


def above(k, k_up, speed, e, e_up):
    return (0.5 * (k + k_up) - jnp.minimum(speed, 0.0)) * (e_up - e)


def below(k, k_down, speed, e, e_down):
    return (0.5 * (k + k_down) + jnp.maximum(speed, 0.0)) * (e_down - e)


def kernel(
    sizes, e_hbm, f_hbm, out, mean_ref, run_ref,
    e_v, k_v, u_v, h_v, n_v, group_v, block_v,
    load_sem, s1, r1, s2, r2, s3, r3, own_sem, s4, r4, s5, r5,
):
    gx_n, gy_n, gz_n, planes, nx, ny = sizes
    height, width = nx // gx_n, ny // gy_n
    gx, gy, gz = lax.axis_index("gx"), lax.axis_index("gy"), lax.axis_index("gz")
    peers = gx_n * gy_n
    place = gy * gx_n + gx
    slab = gz * peers + place

    def device(number):
        return {
            "gx": lax.rem(number, gx_n),
            "gy": lax.rem(lax.div(number, gx_n), gy_n),
            "gz": lax.div(number, peers),
        }

    total = peers * gz_n
    up = device(lax.rem(slab + 1, total))
    down = device(lax.rem(slab + total - 1, total))

    def peer(step):
        return {
            "gx": lax.rem(place + step, gx_n) if gy_n == 1 else lax.rem(lax.rem(place + step, peers), gx_n),
            "gy": lax.div(lax.rem(place + step, peers), gx_n),
            "gz": gz,
        }

    def layer(step):
        return {"gx": gx, "gy": gy, "gz": lax.rem(gz + step, gz_n)}

    loads = [
        pltpu.make_async_copy(e_hbm, e_v.at[pl.ds(1, planes), pl.ds(PAD, nx)], load_sem.at[0]),
        pltpu.make_async_copy(f_hbm.at[3], k_v.at[pl.ds(1, planes), pl.ds(PAD, nx)], load_sem.at[1]),
        pltpu.make_async_copy(f_hbm.at[pl.ds(0, 3)], u_v, load_sem.at[2]),
    ]

    barrier = pltpu.get_barrier_semaphore()
    greet = [up, down] + [peer(i) for i in range(1, peers)] + [layer(i) for i in range(1, gz_n)]
    for target in greet:
        pl.semaphore_signal(barrier, inc=1, device_id=target, device_id_type=MESH)
    for load in loads:
        load.start()
    edge = jnp.zeros((planes, PAD, ny), jnp.float32)
    for ref in (e_v, k_v, h_v):
        ref[1 : planes + 1, 0:PAD, :] = edge
        ref[1 : planes + 1, PAD + nx : PAD + nx + PAD, :] = edge
    pl.semaphore_wait(barrier, len(greet))

    def lanes(c):
        return pl.ds(c * width, width)

    def send(src, dst, send_sem, recv_sem, target):
        return pltpu.make_async_remote_copy(
            src_ref=src, dst_ref=dst, send_sem=send_sem, recv_sem=recv_sem,
            device_id=target, device_id_type=MESH,
        )

    first = []
    rows_all = pl.ds(PAD, nx)
    for c in range(gy_n):
        copies = [
            send(e_hbm.at[planes - 1, :, lanes(c)], e_v.at[0, rows_all, lanes(c)], s1.at[c, 0], r1.at[c, 0], up),
            send(e_hbm.at[0, :, lanes(c)], e_v.at[planes + 1, rows_all, lanes(c)], s1.at[c, 1], r1.at[c, 1], down),
            send(f_hbm.at[3, planes - 1, :, lanes(c)], k_v.at[0, rows_all, lanes(c)], s1.at[c, 2], r1.at[c, 2], up),
            send(f_hbm.at[3, 0, :, lanes(c)], k_v.at[planes + 1, rows_all, lanes(c)], s1.at[c, 3], r1.at[c, 3], down),
        ]
        for copy in copies:
            copy.start()
        first.append(copies)

    for load in loads:
        load.wait()

    lane = lax.broadcasted_iota(jnp.int32, (ROWS, ny), 1)

    def local(src, p, r):
        start = pl.multiple_of(r * ROWS, ROWS)
        here = pl.ds(start, ROWS)
        inner = pl.ds(pl.multiple_of(start + PAD, PAD), ROWS)
        tall = pl.ds(start, ROWS + 2 * PAD)
        e, e_next, e_prev = shifted(src[p + 1, tall, :], ROWS)
        k, k_next, k_prev = shifted(k_v[p + 1, tall, :], ROWS)
        speed = u_v[1, p, here, :]
        value = e + above(k, k_next, speed, e, e_next) + below(k, k_prev, speed, e, e_prev)
        e_next, e_prev = sideways(e, lane)
        k_next, k_prev = sideways(k, lane)
        speed = u_v[2, p, here, :]
        value = value + above(k, k_next, speed, e, e_next) + below(k, k_prev, speed, e, e_prev)
        speed = u_v[0, p, here, :]
        if p < planes - 1:
            value = value + above(k, k_v[p + 2, inner, :], speed, e, src[p + 2, inner, :])
        if p > 0:
            value = value + below(k, k_v[p, inner, :], speed, e, src[p, inner, :])
        return here, inner, value

    def edge_terms(src, c, r):
        start = pl.multiple_of(r * STRIP, STRIP)
        here = pl.ds(start, STRIP)
        inner = pl.ds(pl.multiple_of(start + PAD, PAD), STRIP)
        at = lanes(c)
        top = above(
            k_v[planes, inner, at], k_v[planes + 1, inner, at], u_v[0, planes - 1, here, at],
            src[planes, inner, at], src[planes + 1, inner, at],
        )
        bottom = below(
            k_v[1, inner, at], k_v[0, inner, at], u_v[0, 0, here, at], src[1, inner, at], src[0, inner, at]
        )
        return here, inner, top, bottom

    def folded(value):
        rows = value.shape[0]
        part = value[0:8]
        for i in range(8, rows, 8):
            part = part + value[i : i + 8]
        return part

    for p in range(planes):

        @pl.loop(0, nx // ROWS)
        def _(r, p=p):
            here, inner, value = local(e_v, p, r)
            h_v[p + 1, inner, :] = value

    second = []
    for c in range(gy_n):
        for copy in first[c]:
            copy.wait_recv()

        @pl.loop(0, nx // STRIP)
        def _(r, c=c):
            here, inner, top, bottom = edge_terms(e_v, c, r)
            h_v[planes, inner, lanes(c)] = h_v[planes, inner, lanes(c)] + top
            h_v[1, inner, lanes(c)] = h_v[1, inner, lanes(c)] + bottom

        copies = [
            send(h_v.at[planes, rows_all, lanes(c)], h_v.at[0, rows_all, lanes(c)], s2.at[c, 0], r2.at[c, 0], up),
            send(h_v.at[1, rows_all, lanes(c)], h_v.at[planes + 1, rows_all, lanes(c)], s2.at[c, 1], r2.at[c, 1], down),
        ]
        for copy in copies:
            copy.start()
        second.append(copies)

    sums = []
    for p in range(planes):

        def body(r, carry, p=p):
            here, inner, value = local(h_v, p, r)
            n_v[p, here, :] = value
            return carry + folded(value)

        sums.append(lax.fori_loop(0, nx // ROWS, body, jnp.zeros((8, ny), jnp.float32)))

    def hand_out(c, p0, count, part):
        for d in range(gx_n):
            to = lax.rem(gx + d, gx_n)
            src = n_v.at[pl.ds(p0, count), pl.ds(pl.multiple_of(to * height, 8), height), lanes(c)]
            dst = out.at[pl.ds(place * planes + p0, count)]
            if d == 0:

                @pl.when(gy == c)
                def _():
                    pltpu.make_async_copy(src, dst, own_sem.at[part]).start()

                @pl.when(gy != c)
                def _():
                    send(src, dst, s3.at[c * gx_n + d, part], r3.at[place, part],
                         {"gx": gx, "gy": jnp.int32(c), "gz": gz}).start()
            else:
                send(src, dst, s3.at[c * gx_n + d, part], r3.at[place, part],
                     {"gx": to, "gy": jnp.int32(c), "gz": gz}).start()

    parts = []
    if planes > 2:
        parts.append((1, planes - 2))
        for c in range(gy_n):
            hand_out(c, 1, planes - 2, 0)
    outer = sorted({0, planes - 1})
    first_outer = len(parts)
    parts += [(p, 1) for p in outer]

    extra = [jnp.zeros((8, width), jnp.float32), jnp.zeros((8, width), jnp.float32)]
    for c in range(gy_n):
        for copy in second[c]:
            copy.wait_recv()

        def body(r, carry, c=c):
            here, inner, top, bottom = edge_terms(h_v, c, r)
            n_v[planes - 1, here, lanes(c)] = n_v[planes - 1, here, lanes(c)] + top
            n_v[0, here, lanes(c)] = n_v[0, here, lanes(c)] + bottom
            return carry[0] + folded(top), carry[1] + folded(bottom)

        extra = lax.fori_loop(0, nx // STRIP, body, tuple(extra))
        for part, p in enumerate(outer):
            hand_out(c, p, 1, first_outer + part)

    spot = lax.broadcasted_iota(jnp.int32, (8, 128), 1)
    mine = jnp.zeros((8, 128), jnp.float32)
    for p in range(planes):
        amount = jnp.sum(sums[p], keepdims=True)
        if p == planes - 1:
            amount = amount + jnp.sum(extra[0], keepdims=True)
        if p == 0:
            amount = amount + jnp.sum(extra[1], keepdims=True)
        mine = jnp.where(spot == place * planes + p, amount * (1.0 / (nx * ny)), mine)
    group_v[0] = mine
    share = []
    for i in range(1, peers):
        copy = send(group_v.at[0], group_v.at[i], s4.at[i], r4.at[i], peer(i))
        copy.start()
        share.append(copy)
    for copy in share:
        copy.wait_recv()
    means = mine
    for i in range(1, peers):
        means = means + group_v[i]
    block_v[0] = means
    climb = []
    for i in range(1, gz_n):
        copy = send(block_v.at[0], block_v.at[i], s5.at[i], r5.at[i], layer(i))
        copy.start()
        climb.append(copy)
    running = means
    step = 1
    while step < peers * planes:
        running = running + jnp.where(spot >= step, pltpu.roll(running, step, 1), 0.0)
        step *= 2
    mean_ref[...] = means
    for copy in climb:
        copy.wait_recv()
    lower = jnp.zeros((8, 128), jnp.float32)
    for i in range(1, gz_n):
        lower = lower + jnp.where(gz >= i, block_v[i], 0.0)
    offset = jnp.sum(lower[0:1], axis=1, keepdims=True)
    rank = (gz * peers * planes + spot + 1).astype(jnp.float32)
    run_ref[...] = (running + offset) / rank

    for part, (p0, count) in enumerate(parts):
        for d in range(peers):
            source = lax.rem(place + d, peers)
            dst = out.at[pl.ds(source * planes + p0, count)]
            src = n_v.at[pl.ds(p0, count), pl.ds(0, height), pl.ds(0, width)]
            if d == 0:
                pltpu.make_async_copy(src, dst, own_sem.at[part]).wait()
            else:
                send(src, dst, s3.at[0, part], r3.at[source, part], peer(d)).wait_recv()
        for c in range(gy_n):
            for d in range(gx_n):
                copy = send(
                    n_v.at[pl.ds(p0, count), pl.ds(0, height), pl.ds(0, width)],
                    out.at[pl.ds(p0, count)], s3.at[c * gx_n + d, part], r3.at[0, part], up,
                )
                if d == 0:

                    @pl.when(gy != c)
                    def _():
                        copy.wait_send()
                else:
                    copy.wait_send()
    for copies in first + second + [share, climb]:
        for copy in copies:
            copy.wait_send()


def face_kernel(
    sizes, e_hbm, f_hbm, out, mean_ref, run_ref,
    x_v, h_v, n_v, g_v, rx_v, d_v, c_v, near_v, far_v, corr, spill_v, fixed_v, group_v, block_v,
    load_sem, s1, r1, s2, r2, s3, r3, s4, r4, s5, r5, s6, r6, s7, r7, known, higher, lower,
):
    gx_n, gy_n, gz_n, planes, nx, ny = sizes
    height, width = nx // gx_n, ny // gy_n
    halves = gx_n // 2
    deep = planes // 2
    gx, gy, gz = lax.axis_index("gx"), lax.axis_index("gy"), lax.axis_index("gz")
    peers = gx_n * gy_n
    count = peers * planes
    place = gy * gx_n + gx
    slab = gz * peers + place
    parity = lax.rem(gx, 2)
    total = peers * gz_n
    last = planes - 1

    def device(number):
        return {
            "gx": lax.rem(number, gx_n),
            "gy": lax.rem(lax.div(number, gx_n), gy_n),
            "gz": lax.div(number, peers),
        }

    def peer(step):
        return device(gz * peers + lax.rem(place + step, peers))

    def layer(step):
        return {"gx": gx, "gy": gy, "gz": lax.rem(gz + step, gz_n)}

    side = (1 - parity, parity)
    sign = tuple((1 - 2 * s).astype(jnp.float32) for s in side)
    far_slab = tuple(lax.rem(slab + total + 2 * s - 1, total) for s in side)
    neighbour = tuple(device(s) for s in far_slab)
    group = tuple(s * deep for s in side)

    crossing = lax.div(far_slab[1], peers) != gz
    e_v, k_v = x_v.at[0], x_v.at[1]

    def plane(w, t):
        return t + side[w] * (last - 2 * t)

    half_row = lax.div(gx, 2)

    def turn(first, i):
        return lax.rem(first + 1 + i, halves)

    theirs = [2 * turn(half_row, i) + 1 - parity for i in range(halves)]
    mine = [
        [2 * turn(lax.div(lax.rem(far_slab[w], gx_n), 2), i) + parity for i in range(halves)] for w in (0, 1)
    ]

    inner = tuple(group[w] + 1 - side[w] for w in (0, 1))
    rows_all = pl.ds(PAD, nx)

    def load_planes(fields, p, some, semaphore):
        for field in fields:
            source = e_hbm.at[pl.ds(p, some)] if field == 0 else f_hbm.at[(field + 2) % 4, pl.ds(p, some)]
            pltpu.make_async_copy(source, x_v.at[field, pl.ds(p, some), rows_all], load_sem.at[semaphore]).start()

    def landed(first, fields, p, some, semaphore):
        part = x_v.at[pl.ds(first, fields), pl.ds(p, some), rows_all]
        pltpu.make_async_copy(part, part, load_sem.at[semaphore]).wait()

    barrier = pltpu.get_barrier_semaphore()
    def signal(semaphore, target):
        pl.semaphore_signal(semaphore, inc=1, device_id=target, device_id_type=MESH)

    pair = {"gx": gx + 1 - 2 * parity, "gy": gy, "gz": gz}
    lines = [(half_row + i < halves, {"gx": lax.rem(gx + 2 * i, gx_n), "gy": gy, "gz": gz}) for i in range(1, halves)]
    lines += [(gy - i >= 0, {"gx": gx, "gy": lax.rem(gy + gy_n - i, gy_n), "gz": gz}) for i in range(1, gy_n)]
    earlier = half_row + gy_n - 1 - gy
    later = halves - 1 - half_row + gy
    signal(barrier, pair)
    for after, target in lines + [(gz + i < gz_n, layer(i)) for i in range(1, gz_n)]:

        @pl.when(after)
        def _():
            signal(barrier, target)

    load_planes((0, 1), plane(0, 0), 1, 0)
    load_planes((0, 1), inner[0], deep - 1, 1)
    load_planes((2, 3, 4), group[0], deep, 2)
    edge = jnp.zeros((planes, PAD, ny), jnp.float32)
    for ref in (x_v.at[0], x_v.at[1], h_v):
        ref[:, 0:PAD, :] = edge
        ref[:, PAD + nx : PAD + nx + PAD, :] = edge
    block_v[...] = jnp.zeros(block_v.shape, jnp.float32)

    def entry_barrier():
        pl.semaphore_wait(barrier, 1 + earlier + gz)

    entry_barrier()

    def lanes(c):
        return pl.ds(c * width, width)

    def send(src, dst, send_sem, recv_sem, target):
        return pltpu.make_async_remote_copy(
            src_ref=src, dst_ref=dst, send_sem=send_sem, recv_sem=recv_sem,
            device_id=target, device_id_type=MESH,
        )

    def row(block, extra=0):
        return pl.multiple_of(block * height + extra, 8)

    def start_first(w, i, fields, staged=False):
        p, rows = plane(w, 0), pl.ds(row(theirs[i]), height)
        inner = pl.ds(row(theirs[i], PAD), height)
        sources = (e_hbm.at[p, rows], f_hbm.at[3, p, rows], g_v.at[w, rows], h_v.at[p, inner])
        if staged:
            sources = (x_v.at[0, p, inner], x_v.at[1, p, inner])
        for field in fields:
            send(sources[field], rx_v.at[w, i, field], s1.at[w], r1.at[w, i], neighbour[w]).start()

    @pl.when(parity == 0)
    def _():
        landed(0, 2, plane(0, 0), 1, 0)
        for i in range(halves):
            start_first(0, i, (0, 1), True)

    @pl.when(parity > 0)
    def _():
        for i in range(halves):
            start_first(0, i, (0, 1))
        landed(0, 2, plane(0, 0), 1, 0)

    for after, target in lines:

        @pl.when(jnp.logical_not(after))
        def _():
            signal(known.at[0], target)

    load_planes(range(5), group[1], deep, 3)

    def hear(stage, amount):
        @pl.when(amount > 0)
        def _():
            pl.semaphore_wait(known.at[stage], amount)

    def pass_on(stage):
        for target in [pair] + [target for _, target in lines]:
            signal(known.at[stage], target)

    lane = lax.broadcasted_iota(jnp.int32, (ROWS, ny), 1)
    tiles = height // ROWS

    def inplane(src, p, start):
        here = pl.ds(start, ROWS)
        inner = pl.ds(pl.multiple_of(start + PAD, 8), ROWS)
        tall = pl.ds(start, ROWS + 2 * PAD)
        e, e_next, e_prev = shifted(src[p, tall, :], ROWS)
        k, k_next, k_prev = shifted(k_v[p, tall, :], ROWS)
        speed = x_v[3, p, inner, :]
        value = e + above(k, k_next, speed, e, e_next) + below(k, k_prev, speed, e, e_prev)
        e_next, e_prev = sideways(e, lane)
        k_next, k_prev = sideways(k, lane)
        speed = x_v[4, p, inner, :]
        value = value + above(k, k_next, speed, e, e_next) + below(k, k_prev, speed, e, e_prev)
        return here, inner, value, e, k, x_v[2, p, inner, :]

    def at_face(src, w, start):
        p, q = plane(w, 0), plane(w, 1)
        here, inner, value, e, k, speed = inplane(src, p, start)
        speed = sign[w] * speed
        value = value + below(k, k_v[q, inner, :], -speed, e, src[q, inner, :])
        return here, inner, value, k, speed

    def inside(src, p, start):
        here, inner, value, e, k, speed = inplane(src, p, start)
        value = value + above(k, k_v[p + 1, inner, :], speed, e, src[p + 1, inner, :])
        value = value + below(k, k_v[p - 1, inner, :], speed, e, src[p - 1, inner, :])
        return here, inner, value

    def folded(value):
        part = value[0:8]
        for i in range(8, value.shape[0], 8):
            part = part + value[i : i + 8]
        return part

    def first_face(w, block):
        @pl.loop(0, tiles)
        def _(t):
            start = pl.multiple_of(block * height + t * ROWS, 8)
            here, inner, value, k, speed = at_face(e_v, w, start)
            h_v[plane(w, 0), inner, :] = value
            g_v[w, here, :] = 0.5 * k + jnp.maximum(speed, 0.0)

    def hear_higher():
        @pl.when(gz < gz_n - 1)
        def _():
            pl.semaphore_wait(higher, gz_n - 1 - gz)

        for i in range(1, gz_n):

            @pl.when(gz + i < gz_n)
            def _():
                pl.semaphore_signal(lower, inc=1, device_id=layer(i), device_id_type=MESH)

    def hear_lower():
        @pl.when(gz > 0)
        def _():
            pl.semaphore_wait(lower, gz)

    def land(w):
        if w == 0:
            landed(0, 2, inner[0], deep - 1, 1)
            landed(2, 3, group[0], deep, 2)
        else:
            landed(0, 5, group[1], deep, 3)

    land(0)
    first_face(0, theirs[0])
    start_first(0, 0, (2, 3))
    hear(0, later)
    pass_on(1)
    for i in range(1, halves):
        first_face(0, theirs[i])
        start_first(0, i, (2, 3))
    hear(1, 1 + len(lines))
    pass_on(2)
    land(1)
    first_face(1, theirs[0])
    hear(2, 1 + len(lines))
    for i in range(1, gz_n):

        @pl.when(gz - i >= 0)
        def _():
            pl.semaphore_signal(higher, inc=1, device_id=layer(gz_n - i), device_id_type=MESH)


    @pl.when(jnp.logical_not(crossing))
    def _():
        start_first(1, 0, (0, 1, 2, 3))

    for i in range(1, halves):
        first_face(1, theirs[i])
    for w in (0, 1):
        for i in range(halves):
            first_face(w, mine[w][i])
    def inner_planes():
        for p in range(1, last):

            @pl.loop(0, nx // ROWS)
            def _(t, p=p):
                here, inner, value = inside(e_v, p, pl.multiple_of(t * ROWS, 8))
                h_v[p, inner, :] = value

    inner_planes()
    hear_higher()

    zero = jnp.zeros((8, ny), jnp.float32)
    spill = [zero, zero]
    sums = [[zero] * deep for _ in (0, 1)]

    def second_step(w, t, block, i, low, high):
        def body(r, carry):
            start = pl.multiple_of(block * height + r * ROWS, 8)
            if t == 0:
                here, inner, value, k, speed = at_face(h_v, w, start)
                if i is not None:
                    value = value + near_v[w, i, pl.ds(pl.multiple_of(r * ROWS, 8), ROWS), :]
            else:
                here, inner, value = inside(h_v, plane(w, t), start)
            n_v[plane(w, t), here, :] = value
            return carry + folded(value)

        sums[w][t] = lax.fori_loop(low, high, body, sums[w][t])

    def ahead(w, i):
        for t in range(deep):
            second_step(w, t, mine[w][i], i, 0 if t else 1, tiles if t else tiles - 1)

    def behind(w):
        for i in range(halves):
            for t in sorted({0, tiles - 1}):
                second_step(w, 0, mine[w][i], i, t, t + 1)

    def begin(at_home, src, dst, send_sem, recv_sem, target):
        @pl.when(at_home)
        def _():
            pltpu.make_async_copy(src, dst, recv_sem).start()

        @pl.when(jnp.logical_not(at_home))
        def _():
            send(src, dst, send_sem, recv_sem, target).start()

    def fix_copies(w, i):
        far_place, far_block = lax.rem(far_slab[w], peers), lax.div(far_slab[w], peers)
        slot = lax.div(far_place, 2)
        block = mine[w][i]
        for c in range(gy_n):
            at_home = (block == gx) & (gy == c) & (far_block == gz)
            begin(
                at_home, far_v.at[w, i, :, lanes(c)], corr.at[slot, 1 - side[w]], s4, r4,
                {"gx": block, "gy": jnp.int32(c), "gz": far_block},
            )

    def meet_wait(w, i):
        send(rx_v.at[w, i], rx_v.at[w, i], s1.at[w], r1.at[w, i], neighbour[w]).wait_recv()

    def meet_calc(w, i):
        p = plane(w, 0)

        def body(t, carry):
            at = pl.ds(pl.multiple_of(t * ROWS, 8), ROWS)
            start = pl.multiple_of(mine[w][i] * height + t * ROWS, 8)
            here, inner = pl.ds(start, ROWS), pl.ds(pl.multiple_of(start + PAD, 8), ROWS)
            to_near = g_v[w, here, :] + 0.5 * rx_v[w, i, 1, at, :]
            to_far = rx_v[w, i, 2, at, :] + 0.5 * k_v[p, inner, :]
            step = rx_v[w, i, 0, at, :] - e_v[p, inner, :]
            push = to_far * step
            d_v[w, i, at, :] = -push
            here_half = h_v[p, inner, :] + to_near * step
            far_half = rx_v[w, i, 3, at, :] - push
            h_v[p, inner, :] = here_half
            step = far_half - here_half
            near_v[w, i, at, :] = to_near * step
            fix = -(to_far * step)
            far_v[w, i, at, :] = fix
            return carry + folded(fix)

        spill[w] = lax.fori_loop(0, tiles, body, spill[w])

    def meet_send(w, i):
        send(d_v.at[w, i], c_v.at[w, i], s2, r2.at[w, i], neighbour[w]).start()
        fix_copies(w, i)

    def spill_copy(w):
        return send(spill_v.at[w, pl.ds(0, 1)], fixed_v.at[w, pl.ds(0, 1)], s5, r5, neighbour[w])

    def spill_out(w):
        spill_v[w] = jnp.broadcast_to(jnp.sum(spill[w], keepdims=True), (8, 128))
        spill_copy(w).start()

    def give_wait(w, i):
        if i == 0:
            send(rx_v.at[w], rx_v.at[w], s1.at[w], r1.at[w, 0], neighbour[w]).wait_send()
        send(d_v.at[w, i], c_v.at[w, i], s2, r2.at[w, i], neighbour[w]).wait_recv()

    def give_calc(w, i):
        p = plane(w, 0)

        @pl.loop(0, tiles)
        def _(t):
            at = pl.ds(pl.multiple_of(t * ROWS, 8), ROWS)
            inner = pl.ds(pl.multiple_of(theirs[i] * height + t * ROWS + PAD, 8), ROWS)
            h_v[p, inner, :] = h_v[p, inner, :] + c_v[w, i, at, :]

        for t in range(deep):
            second_step(w, t, theirs[i], None, 0, tiles)

    def hand_theirs(w, i):
        for c in range(gy_n):
            send(
                n_v.at[pl.ds(group[w], deep), pl.ds(row(theirs[i]), height), lanes(c)],
                out.at[pl.ds(place * planes + group[w], deep)], s3, r3,
                {"gx": theirs[i], "gy": jnp.int32(c), "gz": gz},
            ).start()

    def mine_piece(w, i, p, some, start, rows):
        for c in range(gy_n):
            at_home = (mine[w][i] == gx) & (gy == c)
            begin(
                at_home,
                n_v.at[pl.ds(p, some), pl.ds(row(mine[w][i], start), rows), lanes(c)],
                out.at[pl.ds(place * planes + p, some), pl.ds(start, rows)],
                s3, r3, {"gx": mine[w][i], "gy": jnp.int32(c), "gz": gz},
            )

    def mine_early(w, i):
        mine_piece(w, i, group[w] + 1 - side[w], deep - 1, 0, height)
        mine_piece(w, i, plane(w, 0), 1, ROWS, height - 2 * ROWS)

    def mine_late(w):
        for i in range(halves):
            mine_piece(w, i, plane(w, 0), 1, 0, ROWS)
            mine_piece(w, i, plane(w, 0), 1, height - ROWS, ROWS)

    def when(condition, act):
        @pl.when(condition)
        def _():
            act()

    inland = jnp.logical_not(crossing)

    def second_faces():
        for i in range(1, halves):
            start_first(1, i, (0, 1, 2, 3))

    def hand_first():
        for i in range(halves - 1):
            hand_theirs(0, i)

    for i in range(halves):
        meet_wait(0, i)
        meet_calc(0, i)
        meet_send(0, i)
    hear_lower()
    when(inland, second_faces)
    when(crossing, lambda: start_first(1, 0, (0, 1, 2, 3)))
    spill_out(0)
    for i in range(halves):
        ahead(0, i)
        mine_early(0, i)
    for i in range(halves):
        if i == halves - 1:
            for j in range(halves):
                give_wait(0, j)
                give_calc(0, j)
            when(inland, hand_first)
            behind(0)
            mine_late(0)
        meet_wait(1, i)
        meet_calc(1, i)
        meet_send(1, i)
        if i == 0:
            when(crossing, second_faces)
        if i < halves - 1:
            ahead(1, i)
            mine_early(1, i)
    spill_out(1)
    when(crossing, hand_first)
    hand_theirs(0, halves - 1)
    ahead(1, halves - 1)
    mine_early(1, halves - 1)
    for i in range(halves):
        give_wait(1, i)
        give_calc(1, i)
    behind(1)

    spot = lax.broadcasted_iota(jnp.int32, (1, 128), 1)
    scale = 1.0 / (nx * ny)
    part = jnp.zeros((1, 128), jnp.float32)
    spilled = spill_v.at[:, pl.ds(0, 1)]
    send(spilled, spilled, s5, r5, neighbour[0]).wait_recv()
    for w in (0, 1):
        for t in range(deep):
            amount = jnp.sum(sums[w][t], keepdims=True)
            if t == 0:
                amount = amount + fixed_v[w, 0:1, 0:1]
            part = jnp.where(spot == place * planes + plane(w, t), amount * scale, part)
    group_v[0, 0:1] = part
    for i in range(1, peers):
        send(group_v.at[0, pl.ds(0, 1)], group_v.at[i, pl.ds(0, 1)], s6, r6, peer(i)).start()
    for i in reversed(range(halves)):
        hand_theirs(1, i)
    mine_late(1)

    others = group_v.at[pl.ds(1, peers - 1), pl.ds(0, 1)]

    def early_sends():
        send(d_v, c_v, s2, r2.at[0, 0], neighbour[0]).wait_send()
        send(spilled, spilled, s5, r5, neighbour[0]).wait_send()

    def share_wait():
        send(others, others, s6, r6, neighbour[0]).wait_recv()

    early_sends()
    share_wait()
    for i in range(1, peers):
        part = part + group_v[i, 0:1]
    block_v[0, 0:1] = part

    def climb_copy(i):
        return send(block_v.at[0, pl.ds(0, 1)], block_v.at[i, pl.ds(0, 1)], s7, r7, layer(i))

    for i in range(1, gz_n):

        @pl.when(gz + i < gz_n)
        def _():
            climb_copy(i).start()

    running = part
    step = 1
    while step < count:
        running = running + jnp.where(spot >= step, pltpu.roll(running, step, 1), 0.0)
        step *= 2
    mean_ref[0:1] = part

    def climb_all():
        for i in range(1, gz_n):

            @pl.when(gz == i)
            def _():
                some = block_v.at[pl.ds(1, i), pl.ds(0, 1)]
                send(some, some, s7, r7, layer(1)).wait_recv()

    climb_all()
    under = block_v[1, 0:1]
    for i in range(2, gz_n):
        under = under + block_v[i, 0:1]
    offset = jnp.sum(jnp.where(spot < count, under, 0.0), axis=1, keepdims=True)
    rank = (gz * count + spot + 1).astype(jnp.float32)
    run_ref[0:1] = (running + offset) / rank

    def final_out():
        send(out, out, s3, r3, neighbour[0]).wait_recv()

    def final_corr():
        send(corr, corr, s4, r4, neighbour[0]).wait_recv()

    final_corr()
    final_out()
    for slot in range(peers // 2):
        start = (2 * slot + 1 - parity) * planes
        for f, p in ((0, 0), (1, last)):
            out[start + p] = out[start + p] + corr[slot, f]

    def final_sends():
        some = out.at[pl.ds(0, (peers - 1) * planes)]
        send(some, some, s3, r3, neighbour[0]).wait_send()
        send(others, others, s6, r6, neighbour[0]).wait_send()
        for n in (0, 1):

            @pl.when(crossing == bool(n))
            def _():
                some = out.at[pl.ds(0, 2 * (halves * gy_n - 1) + n)]
                send(some, some, s4, r4, neighbour[0]).wait_send()

        for i in range(1, gz_n):

            @pl.when(gz == gz_n - 1 - i)
            def _():
                some = block_v.at[pl.ds(0, i), pl.ds(0, 1)]
                send(some, some, s7, r7, layer(1)).wait_send()

    final_sends()


def finish_kernel(base_ref, mean_in, run_in, out_ref, mean_ref, run_ref, mean_v, run_v, done):
    copies = [pltpu.make_async_copy(base_ref, out_ref, done.at[0])]
    copies[0].start()
    count = mean_ref.shape[0]
    for source, staged, target, i in ((mean_in, mean_v, mean_ref, 1), (run_in, run_v, run_ref, 2)):
        staged[...] = source[0, 0:count]
        copies.append(pltpu.make_async_copy(staged, target, done.at[i]))
        copies[i].start()
    for copy in copies:
        copy.wait()


def by_faces(energy, flow):
    gx_n, gy_n, gz_n = (lax.axis_size(a) for a in ("gx", "gy", "gz"))
    planes, nx, ny = energy.shape
    peers, halves = gx_n * gy_n, gx_n // 2
    height, width = nx // gx_n, ny // gy_n
    dma, regular = pltpu.SemaphoreType.DMA, pltpu.SemaphoreType.REGULAR
    f32 = jnp.float32
    vmem = pl.BlockSpec(memory_space=pltpu.VMEM)
    hbm = pl.BlockSpec(memory_space=pltpu.HBM)
    faces = pltpu.VMEM((2, halves, height, ny), f32)
    energy, flow = (pltpu.with_memory_space_constraint(x, pltpu.HBM) for x in (energy, flow))
    base, means, running = pl.pallas_call(
        functools.partial(face_kernel, (gx_n, gy_n, gz_n, planes, nx, ny)),
        out_shape=(
            jax.ShapeDtypeStruct((planes * peers, height, width), f32),
            jax.ShapeDtypeStruct((8, 128), f32),
            jax.ShapeDtypeStruct((8, 128), f32),
        ),
        in_specs=[hbm, hbm],
        out_specs=(vmem, vmem, vmem),
        scratch_shapes=[
            pltpu.VMEM((5, planes, nx + 2 * PAD, ny), f32), pltpu.VMEM((planes, nx + 2 * PAD, ny), f32),
            pltpu.VMEM((planes, nx, ny), f32), pltpu.VMEM((2, nx, ny), f32),
            pltpu.VMEM((2, halves, 4, height, ny), f32), faces, faces, faces, faces,
            pltpu.VMEM((peers // 2, 2, height, width), f32),
            pltpu.VMEM((2, 8, 128), f32), pltpu.VMEM((2, 8, 128), f32),
            pltpu.VMEM((peers, 8, 128), f32), pltpu.VMEM((gz_n, 8, 128), f32),
            dma((4,)), dma((2,)), dma((2, halves)), dma, dma((2, halves)),
            dma, dma, dma, dma, dma, dma, dma, dma, dma, dma,
            regular((3,)), regular, regular,
        ],
        compiler_params=pltpu.CompilerParams(
            collective_id=0, has_side_effects=True, vmem_limit_bytes=12 * (energy.size + flow.size)
        ),
    )(energy, flow)
    count = planes * peers
    return tuple(pl.pallas_call(
        finish_kernel,
        out_shape=(
            jax.ShapeDtypeStruct((count, height, width), f32),
            jax.ShapeDtypeStruct((count,), f32),
            jax.ShapeDtypeStruct((count,), f32),
        ),
        in_specs=[vmem] * 3,
        out_specs=(hbm, hbm, hbm),
        scratch_shapes=[pltpu.VMEM((count,), f32), pltpu.VMEM((count,), f32), dma((3,))],
        compiler_params=pltpu.CompilerParams(vmem_limit_bytes=12 * (energy.size + flow.size)),
    )(base, means, running))


def per_device(energy, flow):
    gx_n, gy_n, gz_n = (lax.axis_size(a) for a in ("gx", "gy", "gz"))
    planes, nx, ny = energy.shape
    if planes > 3 and planes % 2 == 0 and gx_n % 2 == 0 and gz_n > 1:
        return by_faces(energy, flow)
    peers = gx_n * gy_n
    parts = (1 if planes > 2 else 0) + (2 if planes > 1 else 1)
    dma = pltpu.SemaphoreType.DMA
    f32 = jnp.float32
    anywhere = pl.BlockSpec(memory_space=pl.ANY)
    vmem = pl.BlockSpec(memory_space=pltpu.VMEM)
    tall = pltpu.VMEM((planes + 2, nx + 2 * PAD, ny), f32)
    energy_next, means, running = pl.pallas_call(
        functools.partial(kernel, (gx_n, gy_n, gz_n, planes, nx, ny)),
        out_shape=(
            jax.ShapeDtypeStruct((planes * peers, nx // gx_n, ny // gy_n), f32),
            jax.ShapeDtypeStruct((8, 128), f32),
            jax.ShapeDtypeStruct((8, 128), f32),
        ),
        in_specs=[anywhere, anywhere],
        out_specs=(anywhere, vmem, vmem),
        scratch_shapes=[
            tall, tall, pltpu.VMEM((3, planes, nx, ny), f32), tall,
            pltpu.VMEM((planes, nx, ny), f32),
            pltpu.VMEM((peers, 8, 128), f32), pltpu.VMEM((gz_n, 8, 128), f32),
            dma((3,)), dma((gy_n, 4)), dma((gy_n, 4)), dma((gy_n, 2)), dma((gy_n, 2)),
            dma((peers, parts)), dma((peers, parts)), dma((parts,)),
            dma((peers,)), dma((peers,)), dma((gz_n,)), dma((gz_n,)),
        ],
        compiler_params=pltpu.CompilerParams(collective_id=0, has_side_effects=True),
    )(energy, flow)
    count = planes * peers
    return energy_next, means[0, :count], running[0, :count]


def solution(mesh):
    placed = (P(("gz", "gy", "gx"), None, None), P(None, ("gz", "gy", "gx"), None, None))
    return jax.shard_map(
        per_device,
        mesh=mesh,
        in_specs=placed,
        out_specs=(P("gz", "gx", "gy"), P("gz"), P("gz")),
        check_vma=False,
    )
```

```python
import functools

import jax
import jax.numpy as jnp
from jax import lax
from jax.experimental import pallas as pl
from jax.experimental.pallas import tpu as pltpu
from jax.sharding import PartitionSpec as P

MESH = pl.DeviceIdType.MESH
PAD = 8
ROWS = 16
STRIP = 32


def shifted(block, rows):
    size = block.shape[0]
    return (
        block[PAD : PAD + rows],
        pltpu.roll(block, size - 1, 0)[PAD : PAD + rows],
        pltpu.roll(block, 1, 0)[PAD : PAD + rows],
    )


def sideways(block, lane):
    width = block.shape[1]
    right = jnp.where(lane == width - 1, 0.0, pltpu.roll(block, width - 1, 1))
    left = jnp.where(lane == 0, 0.0, pltpu.roll(block, 1, 1))
    return right, left


def above(k, k_up, speed, e, e_up):
    return (0.5 * (k + k_up) - jnp.minimum(speed, 0.0)) * (e_up - e)


def below(k, k_down, speed, e, e_down):
    return (0.5 * (k + k_down) + jnp.maximum(speed, 0.0)) * (e_down - e)


def kernel(
    sizes, e_hbm, f_hbm, out, mean_ref, run_ref,
    e_v, k_v, u_v, h_v, n_v, group_v, block_v,
    load_sem, s1, r1, s2, r2, s3, r3, own_sem, s4, r4, s5, r5,
):
    gx_n, gy_n, gz_n, planes, nx, ny = sizes
    height, width = nx // gx_n, ny // gy_n
    gx, gy, gz = lax.axis_index("gx"), lax.axis_index("gy"), lax.axis_index("gz")
    peers = gx_n * gy_n
    place = gy * gx_n + gx
    slab = gz * peers + place

    def device(number):
        return {
            "gx": lax.rem(number, gx_n),
            "gy": lax.rem(lax.div(number, gx_n), gy_n),
            "gz": lax.div(number, peers),
        }

    total = peers * gz_n
    up = device(lax.rem(slab + 1, total))
    down = device(lax.rem(slab + total - 1, total))

    def peer(step):
        return {
            "gx": lax.rem(place + step, gx_n) if gy_n == 1 else lax.rem(lax.rem(place + step, peers), gx_n),
            "gy": lax.div(lax.rem(place + step, peers), gx_n),
            "gz": gz,
        }

    def layer(step):
        return {"gx": gx, "gy": gy, "gz": lax.rem(gz + step, gz_n)}

    loads = [
        pltpu.make_async_copy(e_hbm, e_v.at[pl.ds(1, planes), pl.ds(PAD, nx)], load_sem.at[0]),
        pltpu.make_async_copy(f_hbm.at[3], k_v.at[pl.ds(1, planes), pl.ds(PAD, nx)], load_sem.at[1]),
        pltpu.make_async_copy(f_hbm.at[pl.ds(0, 3)], u_v, load_sem.at[2]),
    ]

    barrier = pltpu.get_barrier_semaphore()
    greet = [up, down] + [peer(i) for i in range(1, peers)] + [layer(i) for i in range(1, gz_n)]
    for target in greet:
        pl.semaphore_signal(barrier, inc=1, device_id=target, device_id_type=MESH)
    for load in loads:
        load.start()
    edge = jnp.zeros((planes, PAD, ny), jnp.float32)
    for ref in (e_v, k_v, h_v):
        ref[1 : planes + 1, 0:PAD, :] = edge
        ref[1 : planes + 1, PAD + nx : PAD + nx + PAD, :] = edge
    pl.semaphore_wait(barrier, len(greet))

    def lanes(c):
        return pl.ds(c * width, width)

    def send(src, dst, send_sem, recv_sem, target):
        return pltpu.make_async_remote_copy(
            src_ref=src, dst_ref=dst, send_sem=send_sem, recv_sem=recv_sem,
            device_id=target, device_id_type=MESH,
        )

    first = []
    rows_all = pl.ds(PAD, nx)
    for c in range(gy_n):
        copies = [
            send(e_hbm.at[planes - 1, :, lanes(c)], e_v.at[0, rows_all, lanes(c)], s1.at[c, 0], r1.at[c, 0], up),
            send(e_hbm.at[0, :, lanes(c)], e_v.at[planes + 1, rows_all, lanes(c)], s1.at[c, 1], r1.at[c, 1], down),
            send(f_hbm.at[3, planes - 1, :, lanes(c)], k_v.at[0, rows_all, lanes(c)], s1.at[c, 2], r1.at[c, 2], up),
            send(f_hbm.at[3, 0, :, lanes(c)], k_v.at[planes + 1, rows_all, lanes(c)], s1.at[c, 3], r1.at[c, 3], down),
        ]
        for copy in copies:
            copy.start()
        first.append(copies)

    for load in loads:
        load.wait()

    lane = lax.broadcasted_iota(jnp.int32, (ROWS, ny), 1)

    def local(src, p, r):
        start = pl.multiple_of(r * ROWS, ROWS)
        here = pl.ds(start, ROWS)
        inner = pl.ds(pl.multiple_of(start + PAD, PAD), ROWS)
        tall = pl.ds(start, ROWS + 2 * PAD)
        e, e_next, e_prev = shifted(src[p + 1, tall, :], ROWS)
        k, k_next, k_prev = shifted(k_v[p + 1, tall, :], ROWS)
        speed = u_v[1, p, here, :]
        value = e + above(k, k_next, speed, e, e_next) + below(k, k_prev, speed, e, e_prev)
        e_next, e_prev = sideways(e, lane)
        k_next, k_prev = sideways(k, lane)
        speed = u_v[2, p, here, :]
        value = value + above(k, k_next, speed, e, e_next) + below(k, k_prev, speed, e, e_prev)
        speed = u_v[0, p, here, :]
        if p < planes - 1:
            value = value + above(k, k_v[p + 2, inner, :], speed, e, src[p + 2, inner, :])
        if p > 0:
            value = value + below(k, k_v[p, inner, :], speed, e, src[p, inner, :])
        return here, inner, value

    def edge_terms(src, c, r):
        start = pl.multiple_of(r * STRIP, STRIP)
        here = pl.ds(start, STRIP)
        inner = pl.ds(pl.multiple_of(start + PAD, PAD), STRIP)
        at = lanes(c)
        top = above(
            k_v[planes, inner, at], k_v[planes + 1, inner, at], u_v[0, planes - 1, here, at],
            src[planes, inner, at], src[planes + 1, inner, at],
        )
        bottom = below(
            k_v[1, inner, at], k_v[0, inner, at], u_v[0, 0, here, at], src[1, inner, at], src[0, inner, at]
        )
        return here, inner, top, bottom

    def folded(value):
        rows = value.shape[0]
        part = value[0:8]
        for i in range(8, rows, 8):
            part = part + value[i : i + 8]
        return part

    for p in range(planes):

        @pl.loop(0, nx // ROWS)
        def _(r, p=p):
            here, inner, value = local(e_v, p, r)
            h_v[p + 1, inner, :] = value

    second = []
    for c in range(gy_n):
        for copy in first[c]:
            copy.wait_recv()

        @pl.loop(0, nx // STRIP)
        def _(r, c=c):
            here, inner, top, bottom = edge_terms(e_v, c, r)
            h_v[planes, inner, lanes(c)] = h_v[planes, inner, lanes(c)] + top
            h_v[1, inner, lanes(c)] = h_v[1, inner, lanes(c)] + bottom

        copies = [
            send(h_v.at[planes, rows_all, lanes(c)], h_v.at[0, rows_all, lanes(c)], s2.at[c, 0], r2.at[c, 0], up),
            send(h_v.at[1, rows_all, lanes(c)], h_v.at[planes + 1, rows_all, lanes(c)], s2.at[c, 1], r2.at[c, 1], down),
        ]
        for copy in copies:
            copy.start()
        second.append(copies)

    sums = []
    for p in range(planes):

        def body(r, carry, p=p):
            here, inner, value = local(h_v, p, r)
            n_v[p, here, :] = value
            return carry + folded(value)

        sums.append(lax.fori_loop(0, nx // ROWS, body, jnp.zeros((8, ny), jnp.float32)))

    def hand_out(c, p0, count, part):
        for d in range(gx_n):
            to = lax.rem(gx + d, gx_n)
            src = n_v.at[pl.ds(p0, count), pl.ds(pl.multiple_of(to * height, 8), height), lanes(c)]
            dst = out.at[pl.ds(place * planes + p0, count)]
            if d == 0:

                @pl.when(gy == c)
                def _():
                    pltpu.make_async_copy(src, dst, own_sem.at[part]).start()

                @pl.when(gy != c)
                def _():
                    send(src, dst, s3.at[c * gx_n + d, part], r3.at[place, part],
                         {"gx": gx, "gy": jnp.int32(c), "gz": gz}).start()
            else:
                send(src, dst, s3.at[c * gx_n + d, part], r3.at[place, part],
                     {"gx": to, "gy": jnp.int32(c), "gz": gz}).start()

    parts = []
    if planes > 2:
        parts.append((1, planes - 2))
        for c in range(gy_n):
            hand_out(c, 1, planes - 2, 0)
    outer = sorted({0, planes - 1})
    first_outer = len(parts)
    parts += [(p, 1) for p in outer]

    extra = [jnp.zeros((8, width), jnp.float32), jnp.zeros((8, width), jnp.float32)]
    for c in range(gy_n):
        for copy in second[c]:
            copy.wait_recv()

        def body(r, carry, c=c):
            here, inner, top, bottom = edge_terms(h_v, c, r)
            n_v[planes - 1, here, lanes(c)] = n_v[planes - 1, here, lanes(c)] + top
            n_v[0, here, lanes(c)] = n_v[0, here, lanes(c)] + bottom
            return carry[0] + folded(top), carry[1] + folded(bottom)

        extra = lax.fori_loop(0, nx // STRIP, body, tuple(extra))
        for part, p in enumerate(outer):
            hand_out(c, p, 1, first_outer + part)

    spot = lax.broadcasted_iota(jnp.int32, (8, 128), 1)
    mine = jnp.zeros((8, 128), jnp.float32)
    for p in range(planes):
        amount = jnp.sum(sums[p], keepdims=True)
        if p == planes - 1:
            amount = amount + jnp.sum(extra[0], keepdims=True)
        if p == 0:
            amount = amount + jnp.sum(extra[1], keepdims=True)
        mine = jnp.where(spot == place * planes + p, amount * (1.0 / (nx * ny)), mine)
    group_v[0] = mine
    share = []
    for i in range(1, peers):
        copy = send(group_v.at[0], group_v.at[i], s4.at[i], r4.at[i], peer(i))
        copy.start()
        share.append(copy)
    for copy in share:
        copy.wait_recv()
    means = mine
    for i in range(1, peers):
        means = means + group_v[i]
    block_v[0] = means
    climb = []
    for i in range(1, gz_n):
        copy = send(block_v.at[0], block_v.at[i], s5.at[i], r5.at[i], layer(i))
        copy.start()
        climb.append(copy)
    running = means
    step = 1
    while step < peers * planes:
        running = running + jnp.where(spot >= step, pltpu.roll(running, step, 1), 0.0)
        step *= 2
    mean_ref[...] = means
    for copy in climb:
        copy.wait_recv()
    lower = jnp.zeros((8, 128), jnp.float32)
    for i in range(1, gz_n):
        lower = lower + jnp.where(gz >= i, block_v[i], 0.0)
    offset = jnp.sum(lower[0:1], axis=1, keepdims=True)
    rank = (gz * peers * planes + spot + 1).astype(jnp.float32)
    run_ref[...] = (running + offset) / rank

    for part, (p0, count) in enumerate(parts):
        for d in range(peers):
            source = lax.rem(place + d, peers)
            dst = out.at[pl.ds(source * planes + p0, count)]
            src = n_v.at[pl.ds(p0, count), pl.ds(0, height), pl.ds(0, width)]
            if d == 0:
                pltpu.make_async_copy(src, dst, own_sem.at[part]).wait()
            else:
                send(src, dst, s3.at[0, part], r3.at[source, part], peer(d)).wait_recv()
        for c in range(gy_n):
            for d in range(gx_n):
                copy = send(
                    n_v.at[pl.ds(p0, count), pl.ds(0, height), pl.ds(0, width)],
                    out.at[pl.ds(p0, count)], s3.at[c * gx_n + d, part], r3.at[0, part], up,
                )
                if d == 0:

                    @pl.when(gy != c)
                    def _():
                        copy.wait_send()
                else:
                    copy.wait_send()
    for copies in first + second + [share, climb]:
        for copy in copies:
            copy.wait_send()


def face_kernel(
    sizes, e_hbm, f_hbm, out, mean_ref, run_ref,
    x_v, h_v, n_v, g_v, rx_v, d_v, c_v, near_v, far_v, corr, spill_v, fixed_v, group_v, block_v,
    load_sem, s1, r1, s2, r2, s3, r3, s4, r4, s5, r5, s6, r6, s7, r7, known, higher, lower,
):
    gx_n, gy_n, gz_n, planes, nx, ny = sizes
    height, width = nx // gx_n, ny // gy_n
    halves = gx_n // 2
    deep = planes // 2
    gx, gy, gz = lax.axis_index("gx"), lax.axis_index("gy"), lax.axis_index("gz")
    peers = gx_n * gy_n
    count = peers * planes
    place = gy * gx_n + gx
    slab = gz * peers + place
    parity = lax.rem(gx, 2)
    total = peers * gz_n
    last = planes - 1

    def device(number):
        return {
            "gx": lax.rem(number, gx_n),
            "gy": lax.rem(lax.div(number, gx_n), gy_n),
            "gz": lax.div(number, peers),
        }

    def peer(step):
        return device(gz * peers + lax.rem(place + step, peers))

    def layer(step):
        return {"gx": gx, "gy": gy, "gz": lax.rem(gz + step, gz_n)}

    side = (1 - parity, parity)
    sign = tuple((1 - 2 * s).astype(jnp.float32) for s in side)
    far_slab = tuple(lax.rem(slab + total + 2 * s - 1, total) for s in side)
    neighbour = tuple(device(s) for s in far_slab)
    group = tuple(s * deep for s in side)

    crossing = lax.div(far_slab[1], peers) != gz
    e_v, k_v = x_v.at[0], x_v.at[1]

    def plane(w, t):
        return t + side[w] * (last - 2 * t)

    half_row = lax.div(gx, 2)

    def turn(first, i):
        return lax.rem(first + 1 + i, halves)

    theirs = [2 * turn(half_row, i) + 1 - parity for i in range(halves)]
    mine = [
        [2 * turn(lax.div(lax.rem(far_slab[w], gx_n), 2), i) + parity for i in range(halves)] for w in (0, 1)
    ]

    inner = tuple(group[w] + 1 - side[w] for w in (0, 1))
    rows_all = pl.ds(PAD, nx)

    def load_planes(fields, p, some, semaphore):
        for field in fields:
            source = e_hbm.at[pl.ds(p, some)] if field == 0 else f_hbm.at[(field + 2) % 4, pl.ds(p, some)]
            pltpu.make_async_copy(source, x_v.at[field, pl.ds(p, some), rows_all], load_sem.at[semaphore]).start()

    def landed(first, fields, p, some, semaphore):
        part = x_v.at[pl.ds(first, fields), pl.ds(p, some), rows_all]
        pltpu.make_async_copy(part, part, load_sem.at[semaphore]).wait()

    barrier = pltpu.get_barrier_semaphore()
    def signal(semaphore, target):
        pl.semaphore_signal(semaphore, inc=1, device_id=target, device_id_type=MESH)

    pair = {"gx": gx + 1 - 2 * parity, "gy": gy, "gz": gz}
    lines = [(half_row + i < halves, {"gx": lax.rem(gx + 2 * i, gx_n), "gy": gy, "gz": gz}) for i in range(1, halves)]
    lines += [(gy - i >= 0, {"gx": gx, "gy": lax.rem(gy + gy_n - i, gy_n), "gz": gz}) for i in range(1, gy_n)]
    earlier = half_row + gy_n - 1 - gy
    later = halves - 1 - half_row + gy
    signal(barrier, pair)
    for after, target in lines + [(gz + i < gz_n, layer(i)) for i in range(1, gz_n)]:

        @pl.when(after)
        def _():
            signal(barrier, target)

    load_planes((0, 1), plane(0, 0), 1, 0)
    load_planes((0, 1), inner[0], deep - 1, 1)
    load_planes((2, 3, 4), group[0], deep, 2)
    edge = jnp.zeros((planes, PAD, ny), jnp.float32)
    for ref in (x_v.at[0], x_v.at[1], h_v):
        ref[:, 0:PAD, :] = edge
        ref[:, PAD + nx : PAD + nx + PAD, :] = edge
    block_v[...] = jnp.zeros(block_v.shape, jnp.float32)

    def entry_barrier():
        pl.semaphore_wait(barrier, 1 + earlier + gz)

    entry_barrier()

    def lanes(c):
        return pl.ds(c * width, width)

    def send(src, dst, send_sem, recv_sem, target):
        return pltpu.make_async_remote_copy(
            src_ref=src, dst_ref=dst, send_sem=send_sem, recv_sem=recv_sem,
            device_id=target, device_id_type=MESH,
        )

    def row(block, extra=0):
        return pl.multiple_of(block * height + extra, 8)

    def start_first(w, i, fields, staged=False):
        p, rows = plane(w, 0), pl.ds(row(theirs[i]), height)
        inner = pl.ds(row(theirs[i], PAD), height)
        sources = (e_hbm.at[p, rows], f_hbm.at[3, p, rows], g_v.at[w, rows], h_v.at[p, inner])
        if staged:
            sources = (x_v.at[0, p, inner], x_v.at[1, p, inner])
        for field in fields:
            send(sources[field], rx_v.at[w, i, field], s1.at[w], r1.at[w, i], neighbour[w]).start()

    @pl.when(parity == 0)
    def _():
        landed(0, 2, plane(0, 0), 1, 0)
        for i in range(halves):
            start_first(0, i, (0, 1), True)

    @pl.when(parity > 0)
    def _():
        for i in range(halves):
            start_first(0, i, (0, 1))
        landed(0, 2, plane(0, 0), 1, 0)

    for after, target in lines:

        @pl.when(jnp.logical_not(after))
        def _():
            signal(known.at[0], target)

    load_planes(range(5), group[1], deep, 3)

    def hear(stage, amount):
        @pl.when(amount > 0)
        def _():
            pl.semaphore_wait(known.at[stage], amount)

    def pass_on(stage):
        for target in [pair] + [target for _, target in lines]:
            signal(known.at[stage], target)

    lane = lax.broadcasted_iota(jnp.int32, (ROWS, ny), 1)
    tiles = height // ROWS

    def inplane(src, p, start):
        here = pl.ds(start, ROWS)
        inner = pl.ds(pl.multiple_of(start + PAD, 8), ROWS)
        tall = pl.ds(start, ROWS + 2 * PAD)
        e, e_next, e_prev = shifted(src[p, tall, :], ROWS)
        k, k_next, k_prev = shifted(k_v[p, tall, :], ROWS)
        speed = x_v[3, p, inner, :]
        value = e + above(k, k_next, speed, e, e_next) + below(k, k_prev, speed, e, e_prev)
        e_next, e_prev = sideways(e, lane)
        k_next, k_prev = sideways(k, lane)
        speed = x_v[4, p, inner, :]
        value = value + above(k, k_next, speed, e, e_next) + below(k, k_prev, speed, e, e_prev)
        return here, inner, value, e, k, x_v[2, p, inner, :]

    def at_face(src, w, start):
        p, q = plane(w, 0), plane(w, 1)
        here, inner, value, e, k, speed = inplane(src, p, start)
        speed = sign[w] * speed
        value = value + below(k, k_v[q, inner, :], -speed, e, src[q, inner, :])
        return here, inner, value, k, speed

    def inside(src, p, start):
        here, inner, value, e, k, speed = inplane(src, p, start)
        value = value + above(k, k_v[p + 1, inner, :], speed, e, src[p + 1, inner, :])
        value = value + below(k, k_v[p - 1, inner, :], speed, e, src[p - 1, inner, :])
        return here, inner, value

    def folded(value):
        part = value[0:8]
        for i in range(8, value.shape[0], 8):
            part = part + value[i : i + 8]
        return part

    def first_face(w, block):
        @pl.loop(0, tiles)
        def _(t):
            start = pl.multiple_of(block * height + t * ROWS, 8)
            here, inner, value, k, speed = at_face(e_v, w, start)
            h_v[plane(w, 0), inner, :] = value
            g_v[w, here, :] = 0.5 * k + jnp.maximum(speed, 0.0)

    def hear_higher():
        @pl.when(gz < gz_n - 1)
        def _():
            pl.semaphore_wait(higher, gz_n - 1 - gz)

        for i in range(1, gz_n):

            @pl.when(gz + i < gz_n)
            def _():
                pl.semaphore_signal(lower, inc=1, device_id=layer(i), device_id_type=MESH)

    def hear_lower():
        @pl.when(gz > 0)
        def _():
            pl.semaphore_wait(lower, gz)

    def land(w):
        if w == 0:
            landed(0, 2, inner[0], deep - 1, 1)
            landed(2, 3, group[0], deep, 2)
        else:
            landed(0, 5, group[1], deep, 3)

    land(0)
    first_face(0, theirs[0])
    start_first(0, 0, (2, 3))
    hear(0, later)
    pass_on(1)
    for i in range(1, halves):
        first_face(0, theirs[i])
        start_first(0, i, (2, 3))
    hear(1, 1 + len(lines))
    pass_on(2)
    land(1)
    first_face(1, theirs[0])
    hear(2, 1 + len(lines))
    for i in range(1, gz_n):

        @pl.when(gz - i >= 0)
        def _():
            pl.semaphore_signal(higher, inc=1, device_id=layer(gz_n - i), device_id_type=MESH)


    @pl.when(jnp.logical_not(crossing))
    def _():
        start_first(1, 0, (0, 1, 2, 3))

    for i in range(1, halves):
        first_face(1, theirs[i])
    for w in (0, 1):
        for i in range(halves):
            first_face(w, mine[w][i])
    def inner_planes():
        for p in range(1, last):

            @pl.loop(0, nx // ROWS)
            def _(t, p=p):
                here, inner, value = inside(e_v, p, pl.multiple_of(t * ROWS, 8))
                h_v[p, inner, :] = value

    inner_planes()
    hear_higher()

    zero = jnp.zeros((8, ny), jnp.float32)
    spill = [zero, zero]
    sums = [[zero] * deep for _ in (0, 1)]

    def second_step(w, t, block, i, low, high):
        def body(r, carry):
            start = pl.multiple_of(block * height + r * ROWS, 8)
            if t == 0:
                here, inner, value, k, speed = at_face(h_v, w, start)
                if i is not None:
                    value = value + near_v[w, i, pl.ds(pl.multiple_of(r * ROWS, 8), ROWS), :]
            else:
                here, inner, value = inside(h_v, plane(w, t), start)
            n_v[plane(w, t), here, :] = value
            return carry + folded(value)

        sums[w][t] = lax.fori_loop(low, high, body, sums[w][t], unroll=True)

    def ahead(w, i):
        for t in range(deep):
            second_step(w, t, mine[w][i], i, 0 if t else 1, tiles if t else tiles - 1)

    def behind(w):
        for i in range(halves):
            for t in sorted({0, tiles - 1}):
                second_step(w, 0, mine[w][i], i, t, t + 1)

    def begin(at_home, src, dst, send_sem, recv_sem, target):
        @pl.when(at_home)
        def _():
            pltpu.make_async_copy(src, dst, recv_sem).start()

        @pl.when(jnp.logical_not(at_home))
        def _():
            send(src, dst, send_sem, recv_sem, target).start()

    def fix_copies(w, i):
        far_place, far_block = lax.rem(far_slab[w], peers), lax.div(far_slab[w], peers)
        slot = lax.div(far_place, 2)
        block = mine[w][i]
        for c in range(gy_n):
            at_home = (block == gx) & (gy == c) & (far_block == gz)
            begin(
                at_home, far_v.at[w, i, :, lanes(c)], corr.at[slot, 1 - side[w]], s4, r4,
                {"gx": block, "gy": jnp.int32(c), "gz": far_block},
            )

    def meet_wait(w, i):
        send(rx_v.at[w, i], rx_v.at[w, i], s1.at[w], r1.at[w, i], neighbour[w]).wait_recv()

    def meet_calc(w, i):
        p = plane(w, 0)

        def body(t, carry):
            at = pl.ds(pl.multiple_of(t * ROWS, 8), ROWS)
            start = pl.multiple_of(mine[w][i] * height + t * ROWS, 8)
            here, inner = pl.ds(start, ROWS), pl.ds(pl.multiple_of(start + PAD, 8), ROWS)
            to_near = g_v[w, here, :] + 0.5 * rx_v[w, i, 1, at, :]
            to_far = rx_v[w, i, 2, at, :] + 0.5 * k_v[p, inner, :]
            step = rx_v[w, i, 0, at, :] - e_v[p, inner, :]
            push = to_far * step
            d_v[w, i, at, :] = -push
            here_half = h_v[p, inner, :] + to_near * step
            far_half = rx_v[w, i, 3, at, :] - push
            h_v[p, inner, :] = here_half
            step = far_half - here_half
            near_v[w, i, at, :] = to_near * step
            fix = -(to_far * step)
            far_v[w, i, at, :] = fix
            return carry + folded(fix)

        spill[w] = lax.fori_loop(0, tiles, body, spill[w])

    def meet_send(w, i):
        send(d_v.at[w, i], c_v.at[w, i], s2, r2.at[w, i], neighbour[w]).start()
        fix_copies(w, i)

    def spill_copy(w):
        return send(spill_v.at[w, pl.ds(0, 1)], fixed_v.at[w, pl.ds(0, 1)], s5, r5, neighbour[w])

    def spill_out(w):
        spill_v[w] = jnp.broadcast_to(jnp.sum(spill[w], keepdims=True), (8, 128))
        spill_copy(w).start()

    def give_wait(w, i):
        if i == 0:
            send(rx_v.at[w], rx_v.at[w], s1.at[w], r1.at[w, 0], neighbour[w]).wait_send()
        send(d_v.at[w, i], c_v.at[w, i], s2, r2.at[w, i], neighbour[w]).wait_recv()

    def give_calc(w, i):
        p = plane(w, 0)

        @pl.loop(0, tiles)
        def _(t):
            at = pl.ds(pl.multiple_of(t * ROWS, 8), ROWS)
            inner = pl.ds(pl.multiple_of(theirs[i] * height + t * ROWS + PAD, 8), ROWS)
            h_v[p, inner, :] = h_v[p, inner, :] + c_v[w, i, at, :]

        for t in range(deep):
            second_step(w, t, theirs[i], None, 0, tiles)

    def hand_theirs(w, i):
        for c in range(gy_n):
            send(
                n_v.at[pl.ds(group[w], deep), pl.ds(row(theirs[i]), height), lanes(c)],
                out.at[pl.ds(place * planes + group[w], deep)], s3, r3,
                {"gx": theirs[i], "gy": jnp.int32(c), "gz": gz},
            ).start()

    def mine_piece(w, i, p, some, start, rows):
        for c in range(gy_n):
            at_home = (mine[w][i] == gx) & (gy == c)
            begin(
                at_home,
                n_v.at[pl.ds(p, some), pl.ds(row(mine[w][i], start), rows), lanes(c)],
                out.at[pl.ds(place * planes + p, some), pl.ds(start, rows)],
                s3, r3, {"gx": mine[w][i], "gy": jnp.int32(c), "gz": gz},
            )

    def mine_early(w, i):
        mine_piece(w, i, group[w] + 1 - side[w], deep - 1, 0, height)
        mine_piece(w, i, plane(w, 0), 1, ROWS, height - 2 * ROWS)

    def mine_late(w):
        for i in range(halves):
            mine_piece(w, i, plane(w, 0), 1, 0, ROWS)
            mine_piece(w, i, plane(w, 0), 1, height - ROWS, ROWS)

    def when(condition, act):
        @pl.when(condition)
        def _():
            act()

    inland = jnp.logical_not(crossing)

    def second_faces():
        for i in range(1, halves):
            start_first(1, i, (0, 1, 2, 3))

    def hand_first():
        for i in range(1, halves):
            hand_theirs(0, i)

    for i in range(halves):
        meet_wait(0, i)
        meet_calc(0, i)
        meet_send(0, i)
    hear_lower()
    when(inland, second_faces)
    when(crossing, lambda: start_first(1, 0, (0, 1, 2, 3)))
    spill_out(0)
    for i in range(halves):
        ahead(0, i)
        mine_early(0, i)
    for i in range(halves):
        if i == halves - 1:
            for j in range(halves):
                give_wait(0, j)
                give_calc(0, j)
            when(inland, hand_first)
            behind(0)
            mine_late(0)
        meet_wait(1, i)
        meet_calc(1, i)
        meet_send(1, i)
        if i == 0:
            when(crossing, second_faces)
        if i < halves - 1:
            ahead(1, i)
            mine_early(1, i)
    spill_out(1)
    when(crossing, hand_first)
    hand_theirs(0, 0)
    ahead(1, halves - 1)
    mine_early(1, halves - 1)
    for i in range(halves):
        give_wait(1, i)
        give_calc(1, i)
    behind(1)

    spot = lax.broadcasted_iota(jnp.int32, (1, 128), 1)
    scale = 1.0 / (nx * ny)
    part = jnp.zeros((1, 128), jnp.float32)
    spilled = spill_v.at[:, pl.ds(0, 1)]
    send(spilled, spilled, s5, r5, neighbour[0]).wait_recv()
    for w in (0, 1):
        for t in range(deep):
            amount = jnp.sum(sums[w][t], keepdims=True)
            if t == 0:
                amount = amount + fixed_v[w, 0:1, 0:1]
            part = jnp.where(spot == place * planes + plane(w, t), amount * scale, part)
    group_v[0, 0:1] = part
    for i in range(1, peers):
        send(group_v.at[0, pl.ds(0, 1)], group_v.at[i, pl.ds(0, 1)], s6, r6, peer(i)).start()
    def hand_second(order):
        for i in order:
            hand_theirs(1, i)

    between = lax.rem(gx + half_row, 2) == 1
    when(between, lambda: hand_second(range(halves)))
    when(jnp.logical_not(between), lambda: hand_second(reversed(range(halves))))
    mine_late(1)

    others = group_v.at[pl.ds(1, peers - 1), pl.ds(0, 1)]

    def early_sends():
        send(d_v, c_v, s2, r2.at[0, 0], neighbour[0]).wait_send()
        send(spilled, spilled, s5, r5, neighbour[0]).wait_send()

    def share_wait():
        send(others, others, s6, r6, neighbour[0]).wait_recv()

    early_sends()
    share_wait()
    for i in range(1, peers):
        part = part + group_v[i, 0:1]
    block_v[0, 0:1] = part

    def climb_copy(i):
        return send(block_v.at[0, pl.ds(0, 1)], block_v.at[i, pl.ds(0, 1)], s7, r7, layer(i))

    for i in range(1, gz_n):

        @pl.when(gz + i < gz_n)
        def _():
            climb_copy(i).start()

    running = part
    step = 1
    while step < count:
        running = running + jnp.where(spot >= step, pltpu.roll(running, step, 1), 0.0)
        step *= 2
    mean_ref[0:1] = part

    def climb_all():
        for i in range(1, gz_n):

            @pl.when(gz == i)
            def _():
                some = block_v.at[pl.ds(1, i), pl.ds(0, 1)]
                send(some, some, s7, r7, layer(1)).wait_recv()

    climb_all()
    under = block_v[1, 0:1]
    for i in range(2, gz_n):
        under = under + block_v[i, 0:1]
    offset = jnp.sum(jnp.where(spot < count, under, 0.0), axis=1, keepdims=True)
    rank = (gz * count + spot + 1).astype(jnp.float32)
    run_ref[0:1] = (running + offset) / rank

    def final_out():
        send(out, out, s3, r3, neighbour[0]).wait_recv()

    def final_corr():
        send(corr, corr, s4, r4, neighbour[0]).wait_recv()

    final_corr()
    final_out()
    for slot in range(peers // 2):
        start = (2 * slot + 1 - parity) * planes
        for f, p in ((0, 0), (1, last)):
            out[start + p] = out[start + p] + corr[slot, f]

    def final_sends():
        some = out.at[pl.ds(0, (peers - 1) * planes)]
        send(some, some, s3, r3, neighbour[0]).wait_send()
        send(others, others, s6, r6, neighbour[0]).wait_send()
        for n in (0, 1):

            @pl.when(crossing == bool(n))
            def _():
                some = out.at[pl.ds(0, 2 * (halves * gy_n - 1) + n)]
                send(some, some, s4, r4, neighbour[0]).wait_send()

        for i in range(1, gz_n):

            @pl.when(gz == gz_n - 1 - i)
            def _():
                some = block_v.at[pl.ds(0, i), pl.ds(0, 1)]
                send(some, some, s7, r7, layer(1)).wait_send()

    final_sends()


def finish_kernel(base_ref, mean_in, run_in, out_ref, mean_ref, run_ref, mean_v, run_v, done):
    copies = [pltpu.make_async_copy(base_ref, out_ref, done.at[0])]
    copies[0].start()
    count = mean_ref.shape[0]
    for source, staged, target, i in ((mean_in, mean_v, mean_ref, 1), (run_in, run_v, run_ref, 2)):
        staged[...] = source[0, 0:count]
        copies.append(pltpu.make_async_copy(staged, target, done.at[i]))
        copies[i].start()
    for copy in copies:
        copy.wait()


def by_faces(energy, flow):
    gx_n, gy_n, gz_n = (lax.axis_size(a) for a in ("gx", "gy", "gz"))
    planes, nx, ny = energy.shape
    peers, halves = gx_n * gy_n, gx_n // 2
    height, width = nx // gx_n, ny // gy_n
    dma, regular = pltpu.SemaphoreType.DMA, pltpu.SemaphoreType.REGULAR
    f32 = jnp.float32
    vmem = pl.BlockSpec(memory_space=pltpu.VMEM)
    hbm = pl.BlockSpec(memory_space=pltpu.HBM)
    faces = pltpu.VMEM((2, halves, height, ny), f32)
    energy, flow = (pltpu.with_memory_space_constraint(x, pltpu.HBM) for x in (energy, flow))
    base, means, running = pl.pallas_call(
        functools.partial(face_kernel, (gx_n, gy_n, gz_n, planes, nx, ny)),
        out_shape=(
            jax.ShapeDtypeStruct((planes * peers, height, width), f32),
            jax.ShapeDtypeStruct((8, 128), f32),
            jax.ShapeDtypeStruct((8, 128), f32),
        ),
        in_specs=[hbm, hbm],
        out_specs=(vmem, vmem, vmem),
        scratch_shapes=[
            pltpu.VMEM((5, planes, nx + 2 * PAD, ny), f32), pltpu.VMEM((planes, nx + 2 * PAD, ny), f32),
            pltpu.VMEM((planes, nx, ny), f32), pltpu.VMEM((2, nx, ny), f32),
            pltpu.VMEM((2, halves, 4, height, ny), f32), faces, faces, faces, faces,
            pltpu.VMEM((peers // 2, 2, height, width), f32),
            pltpu.VMEM((2, 8, 128), f32), pltpu.VMEM((2, 8, 128), f32),
            pltpu.VMEM((peers, 8, 128), f32), pltpu.VMEM((gz_n, 8, 128), f32),
            dma((4,)), dma((2,)), dma((2, halves)), dma, dma((2, halves)),
            dma, dma, dma, dma, dma, dma, dma, dma, dma, dma,
            regular((3,)), regular, regular,
        ],
        compiler_params=pltpu.CompilerParams(
            collective_id=0, has_side_effects=True, vmem_limit_bytes=12 * (energy.size + flow.size)
        ),
    )(energy, flow)
    count = planes * peers
    return tuple(pl.pallas_call(
        finish_kernel,
        out_shape=(
            jax.ShapeDtypeStruct((count, height, width), f32),
            jax.ShapeDtypeStruct((count,), f32),
            jax.ShapeDtypeStruct((count,), f32),
        ),
        in_specs=[vmem] * 3,
        out_specs=(hbm, hbm, hbm),
        scratch_shapes=[pltpu.VMEM((count,), f32), pltpu.VMEM((count,), f32), dma((3,))],
        compiler_params=pltpu.CompilerParams(vmem_limit_bytes=12 * (energy.size + flow.size)),
    )(base, means, running))


def per_device(energy, flow):
    gx_n, gy_n, gz_n = (lax.axis_size(a) for a in ("gx", "gy", "gz"))
    planes, nx, ny = energy.shape
    if planes > 3 and planes % 2 == 0 and gx_n % 2 == 0 and gz_n > 1:
        return by_faces(energy, flow)
    peers = gx_n * gy_n
    parts = (1 if planes > 2 else 0) + (2 if planes > 1 else 1)
    dma = pltpu.SemaphoreType.DMA
    f32 = jnp.float32
    anywhere = pl.BlockSpec(memory_space=pl.ANY)
    vmem = pl.BlockSpec(memory_space=pltpu.VMEM)
    tall = pltpu.VMEM((planes + 2, nx + 2 * PAD, ny), f32)
    energy_next, means, running = pl.pallas_call(
        functools.partial(kernel, (gx_n, gy_n, gz_n, planes, nx, ny)),
        out_shape=(
            jax.ShapeDtypeStruct((planes * peers, nx // gx_n, ny // gy_n), f32),
            jax.ShapeDtypeStruct((8, 128), f32),
            jax.ShapeDtypeStruct((8, 128), f32),
        ),
        in_specs=[anywhere, anywhere],
        out_specs=(anywhere, vmem, vmem),
        scratch_shapes=[
            tall, tall, pltpu.VMEM((3, planes, nx, ny), f32), tall,
            pltpu.VMEM((planes, nx, ny), f32),
            pltpu.VMEM((peers, 8, 128), f32), pltpu.VMEM((gz_n, 8, 128), f32),
            dma((3,)), dma((gy_n, 4)), dma((gy_n, 4)), dma((gy_n, 2)), dma((gy_n, 2)),
            dma((peers, parts)), dma((peers, parts)), dma((parts,)),
            dma((peers,)), dma((peers,)), dma((gz_n,)), dma((gz_n,)),
        ],
        compiler_params=pltpu.CompilerParams(collective_id=0, has_side_effects=True),
    )(energy, flow)
    count = planes * peers
    return energy_next, means[0, :count], running[0, :count]


def solution(mesh):
    placed = (P(("gz", "gy", "gx"), None, None), P(None, ("gz", "gy", "gx"), None, None))
    return jax.shard_map(
        per_device,
        mesh=mesh,
        in_specs=placed,
        out_specs=(P("gz", "gx", "gy"), P("gz"), P("gz")),
        check_vma=False,
    )
```
